16 devices in a mesh: dp: 4 (over y, z, core), tp: 4 (over x).
Axes of the slice: x: 4, y: 2, z: 1, core: 2. Of those that a mesh axis runs over, the one named last changes fastest.
The devices are a block of a 4x4x8 slice.
Arguments:
- x: bfloat16 [4096, 4096], P(('dp', 'tp')), parts along dimension 0
- w_gate: bfloat16 [4096, 10240], P(None, 'tp')
- w_up: bfloat16 [4096, 10240], P(None, 'tp')
- w_down: bfloat16 [10240, 4096], P('tp')
Outputs:
- output: bfloat16 [4096, 4096], P(('dp', 'tp')), parts along dimension 0
There are 4 independent parts. The reference program is written for one: setup_inputs(seed, part) draws one part's arguments, and reference() takes and returns one part's arrays. A program takes and returns all parts, laid end to end along the dimension named above; an argument that names none is the same for every part.
All inputs are finite; a program needn't handle non-finite values.
Results may differ from the reference program's by a relative error of at most 0.016.
Values are sent between devices in bfloat16 or wider.
A program may use at most 768 MiB of HBM per device.

```python
import jax
import jax.numpy as jnp

ROWS = 1024
D = 4096
FF = 10240


def setup_inputs(seed: int = 0, part: int = 0) -> dict:
    kx, kg, ku, kd = jax.random.split(jax.random.key(seed), 4)
    drawn = {
        "x": jax.random.normal(jax.random.fold_in(kx, part), (ROWS, D), jnp.float32),
        "w_gate": jax.random.normal(kg, (D, FF), jnp.float32) * D**-0.5,
        "w_up": jax.random.normal(ku, (D, FF), jnp.float32) * D**-0.5,
        "w_down": jax.random.normal(kd, (FF, D), jnp.float32) * FF**-0.5,
    }
    return {k: v.astype(jnp.bfloat16) for k, v in drawn.items()}


def reference(x, w_gate, w_up, w_down):
    gate = jnp.dot(x, w_gate, preferred_element_type=jnp.float32)
    up = jnp.dot(x, w_up, preferred_element_type=jnp.float32)
    hidden = (jax.nn.gelu(gate) * up).astype(jnp.bfloat16)
    return jnp.dot(hidden, w_down, preferred_element_type=jnp.float32).astype(jnp.bfloat16)
```

```python
import functools

import jax
import jax.numpy as jnp
from jax import lax
from jax.experimental import pallas as pl
from jax.experimental.pallas import tpu as pltpu
from jax.sharding import PartitionSpec as P

MESH = pl.DeviceIdType.MESH
F32 = jnp.float32
BF16 = jnp.bfloat16

TILE_H = 256
TILE_D = 512
SLOTS_H = 3
SLOTS_D = 3

OWN, FIRST, SECOND, FAR = range(4)


def kernel(
    n,
    x_ref, wg_ref, wu_ref, wd_ref, y_ref,
    xs, hid, wg, wu, wd, own, mid, to_dir, to_far, to_mrg, by_dir, by_far, by_mrg, out,
    x_sem, wg_sem, wu_sem, wd_sem, ag_send, ag_recv, dir_send, dir_recv, far_send, far_recv, mrg_send, mrg_recv, out_sem,
):
    me = lax.axis_index("tp")
    right, left = lax.rem(me + 1, n), lax.rem(me + n - 1, n)
    rows, d = x_ref.shape
    half = rows // 2
    n_h = wg_ref.shape[1] // TILE_H
    n_d = d // TILE_D
    passes = xs.shape[0]
    a, b = pl.ds(0, half), pl.ds(half, half)

    def load_h(g):
        col = pl.ds(pl.multiple_of(lax.rem(g, n_h) * TILE_H, TILE_H), TILE_H)
        s = lax.rem(g, SLOTS_H)
        return (
            pltpu.make_async_copy(wg_ref.at[:, col], wg.at[s], wg_sem.at[s]),
            pltpu.make_async_copy(wu_ref.at[:, col], wu.at[s], wu_sem.at[s]),
        )

    def load_d(g):
        col = pl.ds(pl.multiple_of(lax.rem(g, n_d) * TILE_D, TILE_D), TILE_D)
        s = lax.rem(g, SLOTS_D)
        return pltpu.make_async_copy(wd_ref.at[:, col], wd.at[s], wd_sem.at[s])

    def send(src, dst, send_sem, recv_sem, to):
        return pltpu.make_async_remote_copy(
            src_ref=src, dst_ref=dst, send_sem=send_sem, recv_sem=recv_sem, device_id={"tp": to}, device_id_type=MESH
        )

    own_x = pltpu.make_async_copy(x_ref, xs.at[OWN], x_sem)
    own_x.start()
    for g in range(SLOTS_H):
        for copy in load_h(g):
            copy.start()
    for g in range(SLOTS_D):
        load_d(g).start()

    barrier = pltpu.get_barrier_semaphore()
    for neighbour in (left, right):
        pl.semaphore_signal(barrier, inc=1, device_id={"tp": neighbour}, device_id_type=MESH)
    pl.semaphore_wait(barrier, 2)
    own_x.wait()

    gather = [
        send(xs.at[OWN, a], xs.at[FIRST, a], ag_send.at[0], ag_recv.at[0], right),
        send(xs.at[OWN, b], xs.at[FIRST, b], ag_send.at[1], ag_recv.at[1], left),
        send(xs.at[OWN, b], xs.at[SECOND, a], ag_send.at[2], ag_recv.at[2], right),
        send(xs.at[OWN, a], xs.at[SECOND, b], ag_send.at[3], ag_recv.at[3], left),
        send(xs.at[FIRST, a], xs.at[FAR, a], ag_send.at[4], ag_recv.at[4], right),
        send(xs.at[FIRST, b], xs.at[FAR, b], ag_send.at[5], ag_recv.at[5], left),
    ]
    direct = [
        send(to_dir.at[:, b], by_dir.at[:, b], dir_send.at[0], dir_recv.at[0], right),
        send(to_dir.at[:, a], by_dir.at[:, a], dir_send.at[1], dir_recv.at[1], left),
    ]

    def far(j):
        return (
            send(to_far.at[j, a], by_far.at[j, b], far_send.at[j, 0], far_recv.at[j, 0], right),
            send(to_far.at[j, b], by_far.at[j, a], far_send.at[j, 1], far_recv.at[j, 1], left),
        )

    def merged(j):
        return (
            send(to_mrg.at[j, b], by_mrg.at[j, a], mrg_send.at[j, 0], mrg_recv.at[j, 0], right),
            send(to_mrg.at[j, a], by_mrg.at[j, b], mrg_send.at[j, 1], mrg_recv.at[j, 1], left),
        )

    for copy in gather[:4]:
        copy.start()

    def hidden(p):
        @pl.loop(0, n_h)
        def _(i):
            g = p * n_h + i
            s = lax.rem(g, SLOTS_H)
            for copy in load_h(g):
                copy.wait()
            gate = jnp.dot(xs[p], wg[s], preferred_element_type=F32)
            up = jnp.dot(xs[p], wu[s], preferred_element_type=F32)
            col = pl.ds(pl.multiple_of(i * TILE_H, TILE_H), TILE_H)
            hid[:, col] = (jax.nn.gelu(gate) * up).astype(BF16)

            @pl.when(g + SLOTS_H < passes * n_h)
            def _():
                for copy in load_h(g + SLOTS_H):
                    copy.start()

    def down(p, put):
        @pl.loop(0, n_d)
        def _(j):
            g = p * n_d + j
            s = lax.rem(g, SLOTS_D)
            load_d(g).wait()
            put(j, jnp.dot(hid[...], wd[s], preferred_element_type=F32))

            @pl.when(g + SLOTS_D < passes * n_d)
            def _():
                load_d(g + SLOTS_D).start()

    def put_own(j, term):
        own[j] = term

    def put_direct(j, term):
        to_dir[j] = term.astype(BF16)

    def put_mid(j, term):
        mid[j] = term

    def put_far(j, term):
        to_far[j] = term.astype(BF16)
        for copy in far(j):
            copy.start()

    hidden(OWN)
    down(OWN, put_own)

    for got, onward in zip(gather[0:2], gather[4:6]):
        got.wait_recv()
        onward.start()
    hidden(FIRST)
    down(FIRST, put_direct)
    for copy in direct:
        copy.start()

    for got in gather[2:4]:
        got.wait_recv()
    hidden(SECOND)
    down(SECOND, put_mid)

    for got in gather[4:6]:
        got.wait_recv()
    hidden(FAR)
    down(FAR, put_far)

    @pl.loop(0, n_d)
    def _(j):
        for copy in far(j):
            copy.wait_recv()
        to_mrg[j] = (mid[j] + by_far[j].astype(F32)).astype(BF16)
        for copy in merged(j):
            copy.start()

    for copy in direct:
        copy.wait_recv()

    def write(j):
        col = pl.ds(pl.multiple_of(j * TILE_D, TILE_D), TILE_D)
        return pltpu.make_async_copy(out.at[j], y_ref.at[:, col], out_sem.at[j])

    @pl.loop(0, n_d)
    def _(j):
        for copy in merged(j):
            copy.wait_recv()
        out[j] = (own[j] + by_dir[j].astype(F32) + by_mrg[j].astype(F32)).astype(BF16)
        write(j).start()

    for copy in gather + direct:
        copy.wait_send()

    @pl.loop(0, n_d)
    def _(j):
        for copy in far(j) + merged(j):
            copy.wait_send()
        write(j).wait()


def solution(mesh):
    n = mesh.shape["tp"]

    def step(x, w_gate, w_up, w_down):
        rows, d = x.shape
        ff = w_gate.shape[1]
        n_d = d // TILE_D
        dma = pltpu.SemaphoreType.DMA
        pieces = (n_d, rows, TILE_D)
        return pl.pallas_call(
            functools.partial(kernel, n),
            out_shape=jax.ShapeDtypeStruct((rows, d), BF16),
            in_specs=[pl.BlockSpec(memory_space=pl.ANY)] * 4,
            out_specs=pl.BlockSpec(memory_space=pl.ANY),
            scratch_shapes=[
                pltpu.VMEM((n, rows, d), BF16),
                pltpu.VMEM((rows, ff), BF16),
                pltpu.VMEM((SLOTS_H, d, TILE_H), BF16),
                pltpu.VMEM((SLOTS_H, d, TILE_H), BF16),
                pltpu.VMEM((SLOTS_D, ff, TILE_D), BF16),
                pltpu.VMEM(pieces, F32),
                pltpu.VMEM(pieces, F32),
                pltpu.VMEM(pieces, BF16),
                pltpu.VMEM(pieces, BF16),
                pltpu.VMEM(pieces, BF16),
                pltpu.VMEM(pieces, BF16),
                pltpu.VMEM(pieces, BF16),
                pltpu.VMEM(pieces, BF16),
                pltpu.VMEM(pieces, BF16),
                dma, dma((SLOTS_H,)), dma((SLOTS_H,)), dma((SLOTS_D,)),
                dma((6,)), dma((6,)), dma((2,)), dma((2,)),
                dma((n_d, 2)), dma((n_d, 2)), dma((n_d, 2)), dma((n_d, 2)), dma((n_d,)),
            ],
            compiler_params=pltpu.CompilerParams(
                collective_id=0, has_side_effects=True, vmem_limit_bytes=63 * 1024 * 1024
            ),
            cost_estimate=pl.CostEstimate(
                flops=6 * n * rows * d * ff, bytes_accessed=6 * n * d * ff, transcendentals=n * rows * ff
            ),
            name="mlp_ring",
        )(x, w_gate, w_up, w_down)

    return jax.shard_map(
        step,
        mesh=mesh,
        in_specs=(P(("dp", "tp"), None), P(None, "tp"), P(None, "tp"), P("tp", None)),
        out_specs=P(("dp", "tp"), None),
        check_vma=False,
    )
```

```python
import functools

import jax
import jax.numpy as jnp
from jax import lax
from jax.experimental import pallas as pl
from jax.experimental.pallas import tpu as pltpu
from jax.sharding import PartitionSpec as P

MESH = pl.DeviceIdType.MESH
F32 = jnp.float32
BF16 = jnp.bfloat16

TILE_H = 256
TILE_D = 512
SLOTS_H = 3
SLOTS_D = 3
VMEM_MIB = 54

OWN, FIRST, SECOND, FAR = range(4)


def kernel(
    n,
    x_ref, wg_ref, wu_ref, wd_ref, y_ref,
    xs, hid, wg, wu, wd, own, mid, to_dir, to_far, to_mrg, by_dir, by_far, by_mrg,
    x_sem, wg_sem, wu_sem, wd_sem, ag_send, ag_recv, dir_send, dir_recv, far_send, far_recv, mrg_send, mrg_recv,
):
    me = lax.axis_index("tp")
    right, left = lax.rem(me + 1, n), lax.rem(me + n - 1, n)
    rows, d = x_ref.shape
    half = rows // 2
    n_h = wg_ref.shape[1] // TILE_H
    n_d = d // TILE_D
    passes = xs.shape[0]
    a, b = pl.ds(0, half), pl.ds(half, half)

    def load_h(g):
        col = pl.ds(pl.multiple_of(lax.rem(g, n_h) * TILE_H, TILE_H), TILE_H)
        s = lax.rem(g, SLOTS_H)
        return (
            pltpu.make_async_copy(wg_ref.at[:, col], wg.at[s], wg_sem.at[s]),
            pltpu.make_async_copy(wu_ref.at[:, col], wu.at[s], wu_sem.at[s]),
        )

    def load_d(g):
        col = pl.ds(pl.multiple_of(lax.rem(g, n_d) * TILE_D, TILE_D), TILE_D)
        s = lax.rem(g, SLOTS_D)
        return pltpu.make_async_copy(wd_ref.at[:, col], wd.at[s], wd_sem.at[s])

    def send(src, dst, send_sem, recv_sem, to):
        return pltpu.make_async_remote_copy(
            src_ref=src, dst_ref=dst, send_sem=send_sem, recv_sem=recv_sem, device_id={"tp": to}, device_id_type=MESH
        )

    own_x = pltpu.make_async_copy(x_ref, xs.at[OWN], x_sem)
    own_x.start()
    for g in range(SLOTS_H):
        for copy in load_h(g):
            copy.start()
    for g in range(SLOTS_D):
        load_d(g).start()

    barrier = pltpu.get_barrier_semaphore()
    for neighbour in (left, right):
        pl.semaphore_signal(barrier, inc=1, device_id={"tp": neighbour}, device_id_type=MESH)
    pl.semaphore_wait(barrier, 2)
    own_x.wait()

    gather = [
        send(xs.at[OWN, a], xs.at[FIRST, a], ag_send.at[0], ag_recv.at[0], right),
        send(xs.at[OWN, b], xs.at[FIRST, b], ag_send.at[1], ag_recv.at[1], left),
        send(xs.at[OWN, b], xs.at[SECOND, a], ag_send.at[2], ag_recv.at[2], right),
        send(xs.at[OWN, a], xs.at[SECOND, b], ag_send.at[3], ag_recv.at[3], left),
        send(xs.at[FIRST, a], xs.at[FAR, a], ag_send.at[4], ag_recv.at[4], right),
        send(xs.at[FIRST, b], xs.at[FAR, b], ag_send.at[5], ag_recv.at[5], left),
    ]
    direct = [
        send(to_dir.at[:, b], by_dir.at[:, b], dir_send.at[0], dir_recv.at[0], right),
        send(to_dir.at[:, a], by_dir.at[:, a], dir_send.at[1], dir_recv.at[1], left),
    ]

    def far(j):
        return (
            send(to_far.at[j, a], by_far.at[j, b], far_send.at[j, 0], far_recv.at[j, 0], right),
            send(to_far.at[j, b], by_far.at[j, a], far_send.at[j, 1], far_recv.at[j, 1], left),
        )

    def merged(j):
        return (
            send(to_mrg.at[j, b], by_mrg.at[j, a], mrg_send.at[j, 0], mrg_recv.at[j, 0], right),
            send(to_mrg.at[j, a], by_mrg.at[j, b], mrg_send.at[j, 1], mrg_recv.at[j, 1], left),
        )

    for copy in gather[:4]:
        copy.start()

    def hidden(p):
        @pl.loop(0, n_h)
        def _(i):
            g = p * n_h + i
            s = lax.rem(g, SLOTS_H)
            for copy in load_h(g):
                copy.wait()
            gate = jnp.dot(xs[p], wg[s], preferred_element_type=F32)
            up = jnp.dot(xs[p], wu[s], preferred_element_type=F32)
            col = pl.ds(pl.multiple_of(i * TILE_H, TILE_H), TILE_H)
            hid[:, col] = (jax.nn.gelu(gate) * up).astype(BF16)

            @pl.when(g + SLOTS_H < passes * n_h)
            def _():
                for copy in load_h(g + SLOTS_H):
                    copy.start()

    def down(p, put):
        @pl.loop(0, n_d)
        def _(j):
            g = p * n_d + j
            s = lax.rem(g, SLOTS_D)
            load_d(g).wait()
            put(j, jnp.dot(hid[...], wd[s], preferred_element_type=F32))

            @pl.when(g + SLOTS_D < passes * n_d)
            def _():
                load_d(g + SLOTS_D).start()

    def put_own(j, term):
        own[j] = term

    def put_direct(j, term):
        to_dir[j] = term.astype(BF16)

    def put_mid(j, term):
        mid[j] = term

    def put_far(j, term):
        to_far[j] = term.astype(BF16)
        for copy in far(j):
            copy.start()

    hidden(OWN)
    down(OWN, put_own)

    for got, onward in zip(gather[0:2], gather[4:6]):
        got.wait_recv()
        onward.start()
    hidden(FIRST)
    down(FIRST, put_direct)
    for copy in direct:
        copy.start()

    for got in gather[2:4]:
        got.wait_recv()
    hidden(SECOND)
    down(SECOND, put_mid)

    for got in gather[4:6]:
        got.wait_recv()
    hidden(FAR)
    down(FAR, put_far)

    @pl.loop(0, n_d)
    def _(j):
        for copy in far(j):
            copy.wait_recv()
        to_mrg[j] = (mid[j] + by_far[j].astype(F32)).astype(BF16)
        for copy in merged(j):
            copy.start()

    for copy in direct:
        copy.wait_recv()

    @pl.loop(0, n_d)
    def _(j):
        for copy in merged(j):
            copy.wait_recv()
        col = pl.ds(pl.multiple_of(j * TILE_D, TILE_D), TILE_D)
        y_ref[:, col] = (own[j] + by_dir[j].astype(F32) + by_mrg[j].astype(F32)).astype(BF16)

    for copy in gather + direct:
        copy.wait_send()

    @pl.loop(0, n_d)
    def _(j):
        for copy in far(j) + merged(j):
            copy.wait_send()


def solution(mesh):
    n = mesh.shape["tp"]

    def step(x, w_gate, w_up, w_down):
        rows, d = x.shape
        ff = w_gate.shape[1]
        n_d = d // TILE_D
        dma = pltpu.SemaphoreType.DMA
        pieces = (n_d, rows, TILE_D)
        return pl.pallas_call(
            functools.partial(kernel, n),
            out_shape=pltpu.VMEM((rows, d), BF16),
            in_specs=[pl.BlockSpec(memory_space=pl.ANY)] * 4,
            out_specs=pl.BlockSpec(memory_space=pltpu.VMEM),
            scratch_shapes=[
                pltpu.VMEM((n, rows, d), BF16),
                pltpu.VMEM((rows, ff), BF16),
                pltpu.VMEM((SLOTS_H, d, TILE_H), BF16),
                pltpu.VMEM((SLOTS_H, d, TILE_H), BF16),
                pltpu.VMEM((SLOTS_D, ff, TILE_D), BF16),
                pltpu.VMEM(pieces, F32),
                pltpu.VMEM(pieces, F32),
                pltpu.VMEM(pieces, BF16),
                pltpu.VMEM(pieces, BF16),
                pltpu.VMEM(pieces, BF16),
                pltpu.VMEM(pieces, BF16),
                pltpu.VMEM(pieces, BF16),
                pltpu.VMEM(pieces, BF16),
                dma, dma((SLOTS_H,)), dma((SLOTS_H,)), dma((SLOTS_D,)),
                dma((6,)), dma((6,)), dma((2,)), dma((2,)),
                dma((n_d, 2)), dma((n_d, 2)), dma((n_d, 2)), dma((n_d, 2)),
            ],
            compiler_params=pltpu.CompilerParams(
                collective_id=0, has_side_effects=True, vmem_limit_bytes=VMEM_MIB * 1024 * 1024
            ),
            cost_estimate=pl.CostEstimate(
                flops=6 * n * rows * d * ff, bytes_accessed=6 * n * d * ff, transcendentals=n * rows * ff
            ),
            name="mlp_ring",
        )(x, w_gate, w_up, w_down)

    return jax.shard_map(
        step,
        mesh=mesh,
        in_specs=(P(("dp", "tp"), None), P(None, "tp"), P(None, "tp"), P("tp", None)),
        out_specs=P(("dp", "tp"), None),
        check_vma=False,
    )
```

```python
import functools

import jax
import jax.numpy as jnp
from jax import lax
from jax.experimental import pallas as pl
from jax.experimental.pallas import tpu as pltpu
from jax.sharding import PartitionSpec as P

MESH = pl.DeviceIdType.MESH
F32 = jnp.float32
BF16 = jnp.bfloat16

TILE_H = 256
TILE_D = 512
SLOTS_H = 3
SLOTS_D = 3
VMEM_MIB = 54

OWN, FIRST, SECOND, FAR = range(4)


def kernel(
    n,
    x_ref, wg_ref, wu_ref, wd_ref, y_ref,
    xs, hid, wg, wu, wd, own, mid, to_dir, to_far, to_mrg, by_dir, by_far, by_mrg,
    x_sem, wg_sem, wu_sem, wd_sem, ag_send, ag_recv, dir_send, dir_recv, far_send, far_recv, mrg_send, mrg_recv,
):
    me = lax.axis_index("tp")
    right, left = lax.rem(me + 1, n), lax.rem(me + n - 1, n)
    rows, d = x_ref.shape
    half = rows // 2
    n_h = wg_ref.shape[1] // TILE_H
    n_d = d // TILE_D
    passes = xs.shape[0]
    a, b = pl.ds(0, half), pl.ds(half, half)

    def load_h(g):
        col = pl.ds(pl.multiple_of(lax.rem(g, n_h) * TILE_H, TILE_H), TILE_H)
        s = lax.rem(g, SLOTS_H)
        return (
            pltpu.make_async_copy(wg_ref.at[:, col], wg.at[s], wg_sem.at[s]),
            pltpu.make_async_copy(wu_ref.at[:, col], wu.at[s], wu_sem.at[s]),
        )

    def load_d(g):
        col = pl.ds(pl.multiple_of(lax.rem(g, n_d) * TILE_D, TILE_D), TILE_D)
        s = lax.rem(g, SLOTS_D)
        return pltpu.make_async_copy(wd_ref.at[:, col], wd.at[s], wd_sem.at[s])

    def send(src, dst, send_sem, recv_sem, to):
        return pltpu.make_async_remote_copy(
            src_ref=src, dst_ref=dst, send_sem=send_sem, recv_sem=recv_sem, device_id={"tp": to}, device_id_type=MESH
        )

    own_x = [pltpu.make_async_copy(x_ref.at[h], xs.at[OWN, h], x_sem.at[k]) for k, h in enumerate((a, b))]
    for copy in own_x:
        copy.start()

    barrier = pltpu.get_barrier_semaphore()
    for neighbour in (left, right):
        pl.semaphore_signal(barrier, inc=1, device_id={"tp": neighbour}, device_id_type=MESH)
    pl.semaphore_wait(barrier, 2)

    gather = [
        send(xs.at[OWN, a], xs.at[FIRST, a], ag_send.at[0], ag_recv.at[0], right),
        send(xs.at[OWN, b], xs.at[FIRST, b], ag_send.at[1], ag_recv.at[1], left),
        send(xs.at[OWN, b], xs.at[SECOND, a], ag_send.at[2], ag_recv.at[2], right),
        send(xs.at[OWN, a], xs.at[SECOND, b], ag_send.at[3], ag_recv.at[3], left),
        send(xs.at[FIRST, a], xs.at[FAR, a], ag_send.at[4], ag_recv.at[4], right),
        send(xs.at[FIRST, b], xs.at[FAR, b], ag_send.at[5], ag_recv.at[5], left),
    ]
    direct = [
        send(to_dir.at[:, b], by_dir.at[:, b], dir_send.at[0], dir_recv.at[0], right),
        send(to_dir.at[:, a], by_dir.at[:, a], dir_send.at[1], dir_recv.at[1], left),
    ]

    def far(j):
        return (
            send(to_far.at[j, a], by_far.at[j, b], far_send.at[j, 0], far_recv.at[j, 0], right),
            send(to_far.at[j, b], by_far.at[j, a], far_send.at[j, 1], far_recv.at[j, 1], left),
        )

    def merged(j):
        return (
            send(to_mrg.at[j, b], by_mrg.at[j, a], mrg_send.at[j, 0], mrg_recv.at[j, 0], right),
            send(to_mrg.at[j, a], by_mrg.at[j, b], mrg_send.at[j, 1], mrg_recv.at[j, 1], left),
        )

    own_x[0].wait()
    gather[0].start()
    own_x[1].wait()
    for copy in gather[1:4]:
        copy.start()

    for g in range(SLOTS_H):
        for copy in load_h(g):
            copy.start()
    for g in range(SLOTS_D):
        load_d(g).start()

    def hidden(p):
        @pl.loop(0, n_h)
        def _(i):
            g = p * n_h + i
            s = lax.rem(g, SLOTS_H)
            for copy in load_h(g):
                copy.wait()
            gate = jnp.dot(xs[p], wg[s], preferred_element_type=F32)
            up = jnp.dot(xs[p], wu[s], preferred_element_type=F32)
            col = pl.ds(pl.multiple_of(i * TILE_H, TILE_H), TILE_H)
            hid[:, col] = (jax.nn.gelu(gate) * up).astype(BF16)

            @pl.when(g + SLOTS_H < passes * n_h)
            def _():
                for copy in load_h(g + SLOTS_H):
                    copy.start()

    def down(p, put):
        @pl.loop(0, n_d)
        def _(j):
            g = p * n_d + j
            s = lax.rem(g, SLOTS_D)
            load_d(g).wait()
            put(j, jnp.dot(hid[...], wd[s], preferred_element_type=F32))

            @pl.when(g + SLOTS_D < passes * n_d)
            def _():
                load_d(g + SLOTS_D).start()

    def put_own(j, term):
        own[j] = term

    def put_direct(j, term):
        to_dir[j] = term.astype(BF16)

    def put_mid(j, term):
        mid[j] = term

    def put_far(j, term):
        to_far[j] = term.astype(BF16)
        for copy in far(j):
            copy.start()

    hidden(OWN)
    down(OWN, put_own)

    for got, onward in zip(gather[0:2], gather[4:6]):
        got.wait_recv()
        onward.start()
    hidden(FIRST)
    down(FIRST, put_direct)
    for copy in direct:
        copy.start()

    for got in gather[2:4]:
        got.wait_recv()
    hidden(SECOND)
    down(SECOND, put_mid)

    for got in gather[4:6]:
        got.wait_recv()
    hidden(FAR)
    down(FAR, put_far)

    @pl.loop(0, n_d)
    def _(j):
        for copy in far(j):
            copy.wait_recv()
        to_mrg[j] = (mid[j] + by_far[j].astype(F32)).astype(BF16)
        for copy in merged(j):
            copy.start()

    for copy in direct:
        copy.wait_recv()

    @pl.loop(0, n_d)
    def _(j):
        for copy in merged(j):
            copy.wait_recv()
        col = pl.ds(pl.multiple_of(j * TILE_D, TILE_D), TILE_D)
        y_ref[:, col] = (own[j] + by_dir[j].astype(F32) + by_mrg[j].astype(F32)).astype(BF16)

    for copy in gather + direct:
        copy.wait_send()

    @pl.loop(0, n_d)
    def _(j):
        for copy in far(j) + merged(j):
            copy.wait_send()


def solution(mesh):
    n = mesh.shape["tp"]

    def step(x, w_gate, w_up, w_down):
        rows, d = x.shape
        ff = w_gate.shape[1]
        n_d = d // TILE_D
        dma = pltpu.SemaphoreType.DMA
        pieces = (n_d, rows, TILE_D)
        return pl.pallas_call(
            functools.partial(kernel, n),
            out_shape=pltpu.VMEM((rows, d), BF16),
            in_specs=[pl.BlockSpec(memory_space=pl.ANY)] * 4,
            out_specs=pl.BlockSpec(memory_space=pltpu.VMEM),
            scratch_shapes=[
                pltpu.VMEM((n, rows, d), BF16),
                pltpu.VMEM((rows, ff), BF16),
                pltpu.VMEM((SLOTS_H, d, TILE_H), BF16),
                pltpu.VMEM((SLOTS_H, d, TILE_H), BF16),
                pltpu.VMEM((SLOTS_D, ff, TILE_D), BF16),
                pltpu.VMEM(pieces, F32),
                pltpu.VMEM(pieces, F32),
                pltpu.VMEM(pieces, BF16),
                pltpu.VMEM(pieces, BF16),
                pltpu.VMEM(pieces, BF16),
                pltpu.VMEM(pieces, BF16),
                pltpu.VMEM(pieces, BF16),
                pltpu.VMEM(pieces, BF16),
                dma((2,)), dma((SLOTS_H,)), dma((SLOTS_H,)), dma((SLOTS_D,)),
                dma((6,)), dma((6,)), dma((2,)), dma((2,)),
                dma((n_d, 2)), dma((n_d, 2)), dma((n_d, 2)), dma((n_d, 2)),
            ],
            compiler_params=pltpu.CompilerParams(
                collective_id=0, has_side_effects=True, vmem_limit_bytes=VMEM_MIB * 1024 * 1024
            ),
            cost_estimate=pl.CostEstimate(
                flops=6 * n * rows * d * ff, bytes_accessed=6 * n * d * ff, transcendentals=n * rows * ff
            ),
            name="mlp_ring",
        )(x, w_gate, w_up, w_down)

    return jax.shard_map(
        step,
        mesh=mesh,
        in_specs=(P(("dp", "tp"), None), P(None, "tp"), P(None, "tp"), P("tp", None)),
        out_specs=P(("dp", "tp"), None),
        check_vma=False,
    )
```

```python
import functools

import jax
import jax.numpy as jnp
from jax import lax
from jax.experimental import pallas as pl
from jax.experimental.pallas import tpu as pltpu
from jax.sharding import PartitionSpec as P

MESH = pl.DeviceIdType.MESH
F32 = jnp.float32
BF16 = jnp.bfloat16

TILE_H = 256
TILE_D = 512
SLOTS_H = 3
SLOTS_D = 3
VMEM_MIB = 54
HEAD = 32

OWN, FIRST, SECOND, FAR = range(4)


def kernel(
    n,
    x_ref, wg_ref, wu_ref, wd_ref, y_ref,
    xs, hid, wg, wu, wd, own, mid, to_dir, to_far, to_mrg, by_dir, by_far, by_mrg,
    x_sem, wg_sem, wu_sem, wd_sem, ag_send, ag_recv, dir_send, dir_recv, far_send, far_recv, mrg_send, mrg_recv,
):
    me = lax.axis_index("tp")
    right, left = lax.rem(me + 1, n), lax.rem(me + n - 1, n)
    rows, d = x_ref.shape
    half = rows // 2
    n_h = wg_ref.shape[1] // TILE_H
    n_d = d // TILE_D
    passes = xs.shape[0]
    a, b = pl.ds(0, half), pl.ds(half, half)
    a0, a1 = pl.ds(0, HEAD), pl.ds(HEAD, half - HEAD)
    b0, b1 = pl.ds(half, HEAD), pl.ds(half + HEAD, half - HEAD)

    def load_h(g):
        col = pl.ds(pl.multiple_of(lax.rem(g, n_h) * TILE_H, TILE_H), TILE_H)
        s = lax.rem(g, SLOTS_H)
        return (
            pltpu.make_async_copy(wg_ref.at[:, col], wg.at[s], wg_sem.at[s]),
            pltpu.make_async_copy(wu_ref.at[:, col], wu.at[s], wu_sem.at[s]),
        )

    def load_d(g):
        col = pl.ds(pl.multiple_of(lax.rem(g, n_d) * TILE_D, TILE_D), TILE_D)
        s = lax.rem(g, SLOTS_D)
        return pltpu.make_async_copy(wd_ref.at[:, col], wd.at[s], wd_sem.at[s])

    def send(src, dst, send_sem, recv_sem, to):
        return pltpu.make_async_remote_copy(
            src_ref=src, dst_ref=dst, send_sem=send_sem, recv_sem=recv_sem, device_id={"tp": to}, device_id_type=MESH
        )

    barrier = pltpu.get_barrier_semaphore()
    for neighbour in (left, right):
        pl.semaphore_signal(barrier, inc=1, device_id={"tp": neighbour}, device_id_type=MESH)
    own_x = [pltpu.make_async_copy(x_ref.at[r], xs.at[OWN, r], x_sem.at[k]) for k, r in enumerate((a0, b0, a1, b1))]
    for copy in own_x:
        copy.start()
    pl.semaphore_wait(barrier, 2)

    heads = [
        send(xs.at[OWN, a0], xs.at[FIRST, a0], ag_send.at[0], ag_recv.at[0], right),
        send(xs.at[OWN, b0], xs.at[FIRST, b0], ag_send.at[1], ag_recv.at[1], left),
        send(xs.at[OWN, a1], xs.at[FIRST, a1], ag_send.at[2], ag_recv.at[2], right),
        send(xs.at[OWN, b1], xs.at[FIRST, b1], ag_send.at[3], ag_recv.at[3], left),
    ]
    tails = [
        send(xs.at[OWN, b], xs.at[SECOND, a], ag_send.at[4], ag_recv.at[4], right),
        send(xs.at[OWN, a], xs.at[SECOND, b], ag_send.at[5], ag_recv.at[5], left),
    ]
    onward = [
        send(xs.at[FIRST, a], xs.at[FAR, a], ag_send.at[6], ag_recv.at[6], right),
        send(xs.at[FIRST, b], xs.at[FAR, b], ag_send.at[7], ag_recv.at[7], left),
    ]
    direct = [
        send(to_dir.at[:, b], by_dir.at[:, b], dir_send.at[0], dir_recv.at[0], right),
        send(to_dir.at[:, a], by_dir.at[:, a], dir_send.at[1], dir_recv.at[1], left),
    ]

    def far(j):
        return (
            send(to_far.at[j, a], by_far.at[j, b], far_send.at[j, 0], far_recv.at[j, 0], right),
            send(to_far.at[j, b], by_far.at[j, a], far_send.at[j, 1], far_recv.at[j, 1], left),
        )

    def merged(j):
        return (
            send(to_mrg.at[j, b], by_mrg.at[j, a], mrg_send.at[j, 0], mrg_recv.at[j, 0], right),
            send(to_mrg.at[j, a], by_mrg.at[j, b], mrg_send.at[j, 1], mrg_recv.at[j, 1], left),
        )

    for loaded, copy in zip(own_x, heads):
        loaded.wait()
        copy.start()
    for copy in tails:
        copy.start()

    for g in range(SLOTS_H):
        for copy in load_h(g):
            copy.start()
    for g in range(SLOTS_D):
        load_d(g).start()

    def hidden(p):
        @pl.loop(0, n_h)
        def _(i):
            g = p * n_h + i
            s = lax.rem(g, SLOTS_H)
            for copy in load_h(g):
                copy.wait()
            gate = jnp.dot(xs[p], wg[s], preferred_element_type=F32)
            up = jnp.dot(xs[p], wu[s], preferred_element_type=F32)
            col = pl.ds(pl.multiple_of(i * TILE_H, TILE_H), TILE_H)
            hid[:, col] = (jax.nn.gelu(gate) * up).astype(BF16)

            @pl.when(g + SLOTS_H < passes * n_h)
            def _():
                for copy in load_h(g + SLOTS_H):
                    copy.start()

    def down(p, put):
        @pl.loop(0, n_d)
        def _(j):
            g = p * n_d + j
            s = lax.rem(g, SLOTS_D)
            load_d(g).wait()
            put(j, jnp.dot(hid[...], wd[s], preferred_element_type=F32))

            @pl.when(g + SLOTS_D < passes * n_d)
            def _():
                load_d(g + SLOTS_D).start()

    def put_own(j, term):
        own[j] = term

    def put_direct(j, term):
        to_dir[j] = term.astype(BF16)

    def put_mid(j, term):
        mid[j] = term

    def put_far(j, term):
        to_far[j] = term.astype(BF16)
        for copy in far(j):
            copy.start()

    hidden(OWN)
    down(OWN, put_own)

    for copy in heads:
        copy.wait_recv()
    for copy in onward:
        copy.start()
    hidden(FIRST)
    down(FIRST, put_direct)
    for copy in direct:
        copy.start()

    for copy in tails:
        copy.wait_recv()
    hidden(SECOND)
    down(SECOND, put_mid)

    for copy in onward:
        copy.wait_recv()
    hidden(FAR)
    down(FAR, put_far)

    @pl.loop(0, n_d)
    def _(j):
        for copy in far(j):
            copy.wait_recv()
        to_mrg[j] = (mid[j] + by_far[j].astype(F32)).astype(BF16)
        for copy in merged(j):
            copy.start()

    for copy in direct:
        copy.wait_recv()
    for copy in heads + tails + onward + direct:
        copy.wait_send()

    @pl.loop(0, n_d)
    def _(j):
        for copy in far(j):
            copy.wait_send()

    @pl.loop(0, n_d)
    def _(j):
        for copy in merged(j):
            copy.wait_recv()
        col = pl.ds(pl.multiple_of(j * TILE_D, TILE_D), TILE_D)
        y_ref[:, col] = (own[j] + by_dir[j].astype(F32) + by_mrg[j].astype(F32)).astype(BF16)
        for copy in merged(j):
            copy.wait_send()


def solution(mesh):
    n = mesh.shape["tp"]

    def step(x, w_gate, w_up, w_down):
        rows, d = x.shape
        ff = w_gate.shape[1]
        n_d = d // TILE_D
        dma = pltpu.SemaphoreType.DMA
        pieces = (n_d, rows, TILE_D)
        return pl.pallas_call(
            functools.partial(kernel, n),
            out_shape=pltpu.VMEM((rows, d), BF16),
            in_specs=[pl.BlockSpec(memory_space=pl.ANY)] * 4,
            out_specs=pl.BlockSpec(memory_space=pltpu.VMEM),
            scratch_shapes=[
                pltpu.VMEM((n, rows, d), BF16),
                pltpu.VMEM((rows, ff), BF16),
                pltpu.VMEM((SLOTS_H, d, TILE_H), BF16),
                pltpu.VMEM((SLOTS_H, d, TILE_H), BF16),
                pltpu.VMEM((SLOTS_D, ff, TILE_D), BF16),
                pltpu.VMEM(pieces, F32),
                pltpu.VMEM(pieces, F32),
                pltpu.VMEM(pieces, BF16),
                pltpu.VMEM(pieces, BF16),
                pltpu.VMEM(pieces, BF16),
                pltpu.VMEM(pieces, BF16),
                pltpu.VMEM(pieces, BF16),
                pltpu.VMEM(pieces, BF16),
                dma((4,)), dma((SLOTS_H,)), dma((SLOTS_H,)), dma((SLOTS_D,)),
                dma((8,)), dma((8,)), dma((2,)), dma((2,)),
                dma((n_d, 2)), dma((n_d, 2)), dma((n_d, 2)), dma((n_d, 2)),
            ],
            compiler_params=pltpu.CompilerParams(
                collective_id=0, has_side_effects=True, vmem_limit_bytes=VMEM_MIB * 1024 * 1024
            ),
            cost_estimate=pl.CostEstimate(
                flops=6 * n * rows * d * ff, bytes_accessed=6 * n * d * ff, transcendentals=n * rows * ff
            ),
            name="mlp_ring",
        )(x, w_gate, w_up, w_down)

    return jax.shard_map(
        step,
        mesh=mesh,
        in_specs=(P(("dp", "tp"), None), P(None, "tp"), P(None, "tp"), P("tp", None)),
        out_specs=P(("dp", "tp"), None),
        check_vma=False,
    )
```

```python
import functools

import jax
import jax.numpy as jnp
from jax import lax
from jax.experimental import pallas as pl
from jax.experimental.pallas import tpu as pltpu
from jax.sharding import PartitionSpec as P

MESH = pl.DeviceIdType.MESH
F32 = jnp.float32
BF16 = jnp.bfloat16

TILE_H = 256
TILE_D = 512
SLOTS_H = 3
SLOTS_D = 3
VMEM_MIB = 54
HEAD = 32

OWN, FIRST, SECOND, FAR = range(4)


def kernel(
    n,
    x_ref, wg_ref, wu_ref, wd_ref, y_ref,
    xs, hid, wg, wu, wd, own, mid, to_dir, to_far, to_mrg, by_dir, by_far, by_mrg,
    x_sem, wg_sem, wu_sem, wd_sem, ag_send, ag_recv, dir_send, dir_recv, far_send, far_recv, mrg_send, mrg_recv,
):
    me = lax.axis_index("tp")
    right, left = lax.rem(me + 1, n), lax.rem(me + n - 1, n)
    rows, d = x_ref.shape
    half = rows // 2
    n_h = wg_ref.shape[1] // TILE_H
    n_d = d // TILE_D
    passes = xs.shape[0]
    a, b = pl.ds(0, half), pl.ds(half, half)
    a0, a1 = pl.ds(0, HEAD), pl.ds(HEAD, half - HEAD)
    b0, b1 = pl.ds(half, HEAD), pl.ds(half + HEAD, half - HEAD)

    def load_h(g):
        col = pl.ds(pl.multiple_of(lax.rem(g, n_h) * TILE_H, TILE_H), TILE_H)
        s = lax.rem(g, SLOTS_H)
        return (
            pltpu.make_async_copy(wg_ref.at[:, col], wg.at[s], wg_sem.at[s]),
            pltpu.make_async_copy(wu_ref.at[:, col], wu.at[s], wu_sem.at[s]),
        )

    def load_d(g):
        col = pl.ds(pl.multiple_of(lax.rem(g, n_d) * TILE_D, TILE_D), TILE_D)
        s = lax.rem(g, SLOTS_D)
        return pltpu.make_async_copy(wd_ref.at[:, col], wd.at[s], wd_sem.at[s])

    def send(src, dst, send_sem, recv_sem, to):
        return pltpu.make_async_remote_copy(
            src_ref=src, dst_ref=dst, send_sem=send_sem, recv_sem=recv_sem, device_id={"tp": to}, device_id_type=MESH
        )

    barrier = pltpu.get_barrier_semaphore()
    for neighbour in (left, right):
        pl.semaphore_signal(barrier, inc=1, device_id={"tp": neighbour}, device_id_type=MESH)
    own_x = [pltpu.make_async_copy(x_ref.at[r], xs.at[OWN, r], x_sem.at[k]) for k, r in enumerate((a0, b0, a1, b1))]
    for copy in own_x:
        copy.start()
    pl.semaphore_wait(barrier, 2)

    heads = [
        send(x_ref.at[a0], xs.at[FIRST, a0], ag_send.at[0], ag_recv.at[0], right),
        send(x_ref.at[b0], xs.at[FIRST, b0], ag_send.at[1], ag_recv.at[1], left),
        send(xs.at[OWN, a1], xs.at[FIRST, a1], ag_send.at[2], ag_recv.at[2], right),
        send(xs.at[OWN, b1], xs.at[FIRST, b1], ag_send.at[3], ag_recv.at[3], left),
    ]
    tails = [
        send(xs.at[OWN, b], xs.at[SECOND, a], ag_send.at[4], ag_recv.at[4], right),
        send(xs.at[OWN, a], xs.at[SECOND, b], ag_send.at[5], ag_recv.at[5], left),
    ]
    onward = [
        send(xs.at[FIRST, a], xs.at[FAR, a], ag_send.at[6], ag_recv.at[6], right),
        send(xs.at[FIRST, b], xs.at[FAR, b], ag_send.at[7], ag_recv.at[7], left),
    ]
    direct = [
        send(to_dir.at[:, b], by_dir.at[:, b], dir_send.at[0], dir_recv.at[0], right),
        send(to_dir.at[:, a], by_dir.at[:, a], dir_send.at[1], dir_recv.at[1], left),
    ]

    def far(j):
        return (
            send(to_far.at[j, a], by_far.at[j, b], far_send.at[j, 0], far_recv.at[j, 0], right),
            send(to_far.at[j, b], by_far.at[j, a], far_send.at[j, 1], far_recv.at[j, 1], left),
        )

    def merged(j):
        return (
            send(to_mrg.at[j, b], by_mrg.at[j, a], mrg_send.at[j, 0], mrg_recv.at[j, 0], right),
            send(to_mrg.at[j, a], by_mrg.at[j, b], mrg_send.at[j, 1], mrg_recv.at[j, 1], left),
        )

    for copy in heads[:2]:
        copy.start()
    for copy in own_x:
        copy.wait()
    for copy in heads[2:]:
        copy.start()
    for copy in tails:
        copy.start()

    for g in range(SLOTS_H):
        for copy in load_h(g):
            copy.start()
    for g in range(SLOTS_D):
        load_d(g).start()

    def hidden(p):
        @pl.loop(0, n_h)
        def _(i):
            g = p * n_h + i
            s = lax.rem(g, SLOTS_H)
            for copy in load_h(g):
                copy.wait()
            gate = jnp.dot(xs[p], wg[s], preferred_element_type=F32)
            up = jnp.dot(xs[p], wu[s], preferred_element_type=F32)
            col = pl.ds(pl.multiple_of(i * TILE_H, TILE_H), TILE_H)
            hid[:, col] = (jax.nn.gelu(gate) * up).astype(BF16)

            @pl.when(g + SLOTS_H < passes * n_h)
            def _():
                for copy in load_h(g + SLOTS_H):
                    copy.start()

    def down(p, put):
        @pl.loop(0, n_d)
        def _(j):
            g = p * n_d + j
            s = lax.rem(g, SLOTS_D)
            load_d(g).wait()
            put(j, jnp.dot(hid[...], wd[s], preferred_element_type=F32))

            @pl.when(g + SLOTS_D < passes * n_d)
            def _():
                load_d(g + SLOTS_D).start()

    def put_own(j, term):
        own[j] = term

    def put_direct(j, term):
        to_dir[j] = term.astype(BF16)

    def put_mid(j, term):
        mid[j] = term

    def put_far(j, term):
        to_far[j] = term.astype(BF16)
        for copy in far(j):
            copy.start()

    hidden(OWN)
    down(OWN, put_own)

    for copy in heads:
        copy.wait_recv()
    for copy in onward:
        copy.start()
    hidden(FIRST)
    down(FIRST, put_direct)
    for copy in direct:
        copy.start()

    for copy in tails:
        copy.wait_recv()
    hidden(SECOND)
    down(SECOND, put_mid)

    for copy in onward:
        copy.wait_recv()
    hidden(FAR)
    down(FAR, put_far)

    @pl.loop(0, n_d)
    def _(j):
        for copy in far(j):
            copy.wait_recv()
        to_mrg[j] = (mid[j] + by_far[j].astype(F32)).astype(BF16)
        for copy in merged(j):
            copy.start()

    for copy in direct:
        copy.wait_recv()
    for copy in heads + tails + onward + direct:
        copy.wait_send()

    @pl.loop(0, n_d)
    def _(j):
        for copy in far(j):
            copy.wait_send()

    @pl.loop(0, n_d)
    def _(j):
        for copy in merged(j):
            copy.wait_recv()
        col = pl.ds(pl.multiple_of(j * TILE_D, TILE_D), TILE_D)
        y_ref[:, col] = (own[j] + by_dir[j].astype(F32) + by_mrg[j].astype(F32)).astype(BF16)
        for copy in merged(j):
            copy.wait_send()


def solution(mesh):
    n = mesh.shape["tp"]

    def step(x, w_gate, w_up, w_down):
        rows, d = x.shape
        ff = w_gate.shape[1]
        n_d = d // TILE_D
        dma = pltpu.SemaphoreType.DMA
        pieces = (n_d, rows, TILE_D)
        return pl.pallas_call(
            functools.partial(kernel, n),
            out_shape=pltpu.VMEM((rows, d), BF16),
            in_specs=[pl.BlockSpec(memory_space=pl.ANY)] * 4,
            out_specs=pl.BlockSpec(memory_space=pltpu.VMEM),
            scratch_shapes=[
                pltpu.VMEM((n, rows, d), BF16),
                pltpu.VMEM((rows, ff), BF16),
                pltpu.VMEM((SLOTS_H, d, TILE_H), BF16),
                pltpu.VMEM((SLOTS_H, d, TILE_H), BF16),
                pltpu.VMEM((SLOTS_D, ff, TILE_D), BF16),
                pltpu.VMEM(pieces, F32),
                pltpu.VMEM(pieces, F32),
                pltpu.VMEM(pieces, BF16),
                pltpu.VMEM(pieces, BF16),
                pltpu.VMEM(pieces, BF16),
                pltpu.VMEM(pieces, BF16),
                pltpu.VMEM(pieces, BF16),
                pltpu.VMEM(pieces, BF16),
                dma((4,)), dma((SLOTS_H,)), dma((SLOTS_H,)), dma((SLOTS_D,)),
                dma((8,)), dma((8,)), dma((2,)), dma((2,)),
                dma((n_d, 2)), dma((n_d, 2)), dma((n_d, 2)), dma((n_d, 2)),
            ],
            compiler_params=pltpu.CompilerParams(
                collective_id=0, has_side_effects=True, vmem_limit_bytes=VMEM_MIB * 1024 * 1024
            ),
            cost_estimate=pl.CostEstimate(
                flops=6 * n * rows * d * ff, bytes_accessed=6 * n * d * ff, transcendentals=n * rows * ff
            ),
            name="mlp_ring",
        )(x, w_gate, w_up, w_down)

    return jax.shard_map(
        step,
        mesh=mesh,
        in_specs=(P(("dp", "tp"), None), P(None, "tp"), P(None, "tp"), P("tp", None)),
        out_specs=P(("dp", "tp"), None),
        check_vma=False,
    )
```

```python
import functools

import jax
import jax.numpy as jnp
from jax import lax
from jax.experimental import pallas as pl
from jax.experimental.pallas import tpu as pltpu
from jax.sharding import PartitionSpec as P

MESH = pl.DeviceIdType.MESH
F32 = jnp.float32
BF16 = jnp.bfloat16

TILE_H = 256
TILE_D = 512
SLOTS_H = 3
SLOTS_D = 3
VMEM_MIB = 46
FINISH_MIB = 4
HEAD = 32

OWN, FIRST, SECOND, FAR = range(4)


def kernel(
    n,
    x_ref, wg_ref, wu_ref, wd_ref, y_ref, own, by_mrg,
    xs, hid, wg, wu, wd, mid, to_dir, to_far, to_mrg, by_dir, by_far,
    x_sem, wg_sem, wu_sem, wd_sem, ag_send, ag_recv, dir_send, dir_recv, far_send, far_recv, mrg_send, mrg_recv,
):
    me = lax.axis_index("tp")
    right, left = lax.rem(me + 1, n), lax.rem(me + n - 1, n)
    rows, d = x_ref.shape
    half = rows // 2
    n_h = wg_ref.shape[1] // TILE_H
    n_d = d // TILE_D
    passes = xs.shape[0]
    a, b = pl.ds(0, half), pl.ds(half, half)
    a0, a1 = pl.ds(0, HEAD), pl.ds(HEAD, half - HEAD)
    b0, b1 = pl.ds(half, HEAD), pl.ds(half + HEAD, half - HEAD)

    def load_h(g):
        col = pl.ds(pl.multiple_of(lax.rem(g, n_h) * TILE_H, TILE_H), TILE_H)
        s = lax.rem(g, SLOTS_H)
        return (
            pltpu.make_async_copy(wg_ref.at[:, col], wg.at[s], wg_sem.at[s]),
            pltpu.make_async_copy(wu_ref.at[:, col], wu.at[s], wu_sem.at[s]),
        )

    def load_d(g):
        col = pl.ds(pl.multiple_of(lax.rem(g, n_d) * TILE_D, TILE_D), TILE_D)
        s = lax.rem(g, SLOTS_D)
        return pltpu.make_async_copy(wd_ref.at[:, col], wd.at[s], wd_sem.at[s])

    def send(src, dst, send_sem, recv_sem, to):
        return pltpu.make_async_remote_copy(
            src_ref=src, dst_ref=dst, send_sem=send_sem, recv_sem=recv_sem, device_id={"tp": to}, device_id_type=MESH
        )

    barrier = pltpu.get_barrier_semaphore()
    for neighbour in (left, right):
        pl.semaphore_signal(barrier, inc=1, device_id={"tp": neighbour}, device_id_type=MESH)
    own_x = [pltpu.make_async_copy(x_ref.at[r], xs.at[OWN, r], x_sem.at[k]) for k, r in enumerate((a0, b0, a1, b1))]
    for copy in own_x:
        copy.start()
    pl.semaphore_wait(barrier, 2)

    heads = [
        send(x_ref.at[a0], xs.at[FIRST, a0], ag_send.at[0], ag_recv.at[0], right),
        send(x_ref.at[b0], xs.at[FIRST, b0], ag_send.at[1], ag_recv.at[1], left),
        send(xs.at[OWN, a1], xs.at[FIRST, a1], ag_send.at[2], ag_recv.at[2], right),
        send(xs.at[OWN, b1], xs.at[FIRST, b1], ag_send.at[3], ag_recv.at[3], left),
    ]
    tails = [
        send(xs.at[OWN, b], xs.at[SECOND, a], ag_send.at[4], ag_recv.at[4], right),
        send(xs.at[OWN, a], xs.at[SECOND, b], ag_send.at[5], ag_recv.at[5], left),
    ]
    onward = [
        send(xs.at[FIRST, a], xs.at[FAR, a], ag_send.at[6], ag_recv.at[6], right),
        send(xs.at[FIRST, b], xs.at[FAR, b], ag_send.at[7], ag_recv.at[7], left),
    ]
    direct = [
        send(to_dir.at[:, b], by_dir.at[:, b], dir_send.at[0], dir_recv.at[0], right),
        send(to_dir.at[:, a], by_dir.at[:, a], dir_send.at[1], dir_recv.at[1], left),
    ]

    def far(j):
        return (
            send(to_far.at[j, a], by_far.at[j, b], far_send.at[j, 0], far_recv.at[j, 0], right),
            send(to_far.at[j, b], by_far.at[j, a], far_send.at[j, 1], far_recv.at[j, 1], left),
        )

    def merged(j):
        return (
            send(to_mrg.at[j, b], by_mrg.at[j, a], mrg_send.at[j, 0], mrg_recv.at[j, 0], right),
            send(to_mrg.at[j, a], by_mrg.at[j, b], mrg_send.at[j, 1], mrg_recv.at[j, 1], left),
        )

    for copy in heads[:2]:
        copy.start()
    for copy in own_x:
        copy.wait()
    for copy in heads[2:]:
        copy.start()
    for copy in tails:
        copy.start()

    for g in range(SLOTS_H):
        for copy in load_h(g):
            copy.start()
    for g in range(SLOTS_D):
        load_d(g).start()

    def hidden(p):
        @pl.loop(0, n_h)
        def _(i):
            g = p * n_h + i
            s = lax.rem(g, SLOTS_H)
            for copy in load_h(g):
                copy.wait()
            gate = jnp.dot(xs[p], wg[s], preferred_element_type=F32)
            up = jnp.dot(xs[p], wu[s], preferred_element_type=F32)
            col = pl.ds(pl.multiple_of(i * TILE_H, TILE_H), TILE_H)
            hid[:, col] = (jax.nn.gelu(gate) * up).astype(BF16)

            @pl.when(g + SLOTS_H < passes * n_h)
            def _():
                for copy in load_h(g + SLOTS_H):
                    copy.start()

    def down(p, put):
        @pl.loop(0, n_d)
        def _(j):
            g = p * n_d + j
            s = lax.rem(g, SLOTS_D)
            load_d(g).wait()
            put(j, jnp.dot(hid[...], wd[s], preferred_element_type=F32))

            @pl.when(g + SLOTS_D < passes * n_d)
            def _():
                load_d(g + SLOTS_D).start()

    def put_own(j, term):
        own[j] = term

    def put_direct(j, term):
        to_dir[j] = term.astype(BF16)

    def put_mid(j, term):
        mid[j] = term

    def put_far(j, term):
        to_far[j] = term.astype(BF16)
        for copy in far(j):
            copy.start()

    hidden(OWN)
    down(OWN, put_own)

    for copy in heads:
        copy.wait_recv()
    for copy in onward:
        copy.start()
    hidden(FIRST)
    down(FIRST, put_direct)
    for copy in direct:
        copy.start()

    for copy in tails:
        copy.wait_recv()
    hidden(SECOND)
    down(SECOND, put_mid)

    for copy in onward:
        copy.wait_recv()
    hidden(FAR)
    down(FAR, put_far)

    @pl.loop(0, n_d)
    def _(j):
        for copy in far(j):
            copy.wait_recv()
        to_mrg[j] = (mid[j] + by_far[j].astype(F32)).astype(BF16)
        for copy in merged(j):
            copy.start()

    for copy in direct:
        copy.wait_recv()
    for copy in heads + tails + onward + direct:
        copy.wait_send()

    @pl.loop(0, n_d)
    def _(j):
        for copy in far(j):
            copy.wait_send()

    last = n_d - 1
    own[last] += by_dir[last].astype(F32)

    @pl.loop(0, last)
    def _(j):
        for copy in merged(j):
            copy.wait_recv()
        col = pl.ds(pl.multiple_of(j * TILE_D, TILE_D), TILE_D)
        y_ref[:, col] = (own[j] + by_dir[j].astype(F32) + by_mrg[j].astype(F32)).astype(BF16)
        for copy in merged(j):
            copy.wait_send()

    for copy in merged(last):
        copy.wait_recv()
    for copy in merged(last):
        copy.wait_send()


def finish(y_ref, own, by_mrg, out_ref, piece, sem):
    last = own.shape[0] - 1
    done = pl.ds(0, last * TILE_D)
    rest = pltpu.make_async_copy(y_ref.at[:, done], out_ref.at[:, done], sem.at[0])
    rest.start()
    piece[...] = (own[last] + by_mrg[last].astype(F32)).astype(BF16)
    end = pltpu.make_async_copy(piece, out_ref.at[:, pl.ds(last * TILE_D, TILE_D)], sem.at[1])
    end.start()
    rest.wait()
    end.wait()


def solution(mesh):
    n = mesh.shape["tp"]

    def step(x, w_gate, w_up, w_down):
        rows, d = x.shape
        ff = w_gate.shape[1]
        n_d = d // TILE_D
        dma = pltpu.SemaphoreType.DMA
        pieces = (n_d, rows, TILE_D)
        vmem = pl.BlockSpec(memory_space=pltpu.VMEM)
        parts = pl.pallas_call(
            functools.partial(kernel, n),
            out_shape=(pltpu.VMEM((rows, d), BF16), pltpu.VMEM(pieces, F32), pltpu.VMEM(pieces, BF16)),
            in_specs=[pl.BlockSpec(memory_space=pl.ANY)] * 4,
            out_specs=(vmem, vmem, vmem),
            scratch_shapes=[
                pltpu.VMEM((n, rows, d), BF16),
                pltpu.VMEM((rows, ff), BF16),
                pltpu.VMEM((SLOTS_H, d, TILE_H), BF16),
                pltpu.VMEM((SLOTS_H, d, TILE_H), BF16),
                pltpu.VMEM((SLOTS_D, ff, TILE_D), BF16),
                pltpu.VMEM(pieces, F32),
                pltpu.VMEM(pieces, BF16),
                pltpu.VMEM(pieces, BF16),
                pltpu.VMEM(pieces, BF16),
                pltpu.VMEM(pieces, BF16),
                pltpu.VMEM(pieces, BF16),
                dma((4,)), dma((SLOTS_H,)), dma((SLOTS_H,)), dma((SLOTS_D,)),
                dma((8,)), dma((8,)), dma((2,)), dma((2,)),
                dma((n_d, 2)), dma((n_d, 2)), dma((n_d, 2)), dma((n_d, 2)),
            ],
            compiler_params=pltpu.CompilerParams(
                collective_id=0, has_side_effects=True, vmem_limit_bytes=VMEM_MIB * 1024 * 1024
            ),
            cost_estimate=pl.CostEstimate(
                flops=6 * n * rows * d * ff, bytes_accessed=6 * n * d * ff, transcendentals=n * rows * ff
            ),
            name="mlp_ring",
        )(x, w_gate, w_up, w_down)
        return pl.pallas_call(
            finish,
            out_shape=jax.ShapeDtypeStruct((rows, d), BF16),
            in_specs=[vmem] * 3,
            out_specs=pl.BlockSpec(memory_space=pl.ANY),
            scratch_shapes=[pltpu.VMEM((rows, TILE_D), BF16), dma((2,))],
            compiler_params=pltpu.CompilerParams(vmem_limit_bytes=FINISH_MIB * 1024 * 1024),
            name="finish",
        )(*parts)

    return jax.shard_map(
        step,
        mesh=mesh,
        in_specs=(P(("dp", "tp"), None), P(None, "tp"), P(None, "tp"), P("tp", None)),
        out_specs=P(("dp", "tp"), None),
        check_vma=False,
    )
```

```python
import functools

import jax
import jax.numpy as jnp
from jax import lax
from jax.experimental import pallas as pl
from jax.experimental.pallas import tpu as pltpu
from jax.sharding import PartitionSpec as P

MESH = pl.DeviceIdType.MESH
F32 = jnp.float32
BF16 = jnp.bfloat16

TILE_H = 256
TILE_D = 512
SLOTS_H = 3
SLOTS_D = 3
VMEM_MIB = 46
FINISH_MIB = 4

OWN, FIRST, SECOND, FAR = range(4)


def kernel(
    n,
    x_ref, wg_ref, wu_ref, wd_ref, y_ref, own, by_mrg,
    xs, hid, wg, wu, wd, mid, to_dir, to_far, to_mrg, by_dir, by_far,
    x_sem, wg_sem, wu_sem, wd_sem, ag_send, ag_recv, dir_send, dir_recv, far_send, far_recv, mrg_send, mrg_recv,
):
    me = lax.axis_index("tp")
    right, left = lax.rem(me + 1, n), lax.rem(me + n - 1, n)
    rows, d = x_ref.shape
    half = rows // 2
    n_h = wg_ref.shape[1] // TILE_H
    n_d = d // TILE_D
    passes = xs.shape[0]
    a, b = pl.ds(0, half), pl.ds(half, half)

    def load_h(g):
        col = pl.ds(pl.multiple_of(lax.rem(g, n_h) * TILE_H, TILE_H), TILE_H)
        s = lax.rem(g, SLOTS_H)
        return (
            pltpu.make_async_copy(wg_ref.at[:, col], wg.at[s], wg_sem.at[s]),
            pltpu.make_async_copy(wu_ref.at[:, col], wu.at[s], wu_sem.at[s]),
        )

    def load_d(g):
        col = pl.ds(pl.multiple_of(lax.rem(g, n_d) * TILE_D, TILE_D), TILE_D)
        s = lax.rem(g, SLOTS_D)
        return pltpu.make_async_copy(wd_ref.at[:, col], wd.at[s], wd_sem.at[s])

    def send(src, dst, send_sem, recv_sem, to):
        return pltpu.make_async_remote_copy(
            src_ref=src, dst_ref=dst, send_sem=send_sem, recv_sem=recv_sem, device_id={"tp": to}, device_id_type=MESH
        )

    barrier = pltpu.get_barrier_semaphore()
    for neighbour in (left, right):
        pl.semaphore_signal(barrier, inc=1, device_id={"tp": neighbour}, device_id_type=MESH)
    own_x = pltpu.make_async_copy(x_ref, xs.at[OWN], x_sem)
    own_x.start()
    pl.semaphore_wait(barrier, 2)

    heads = [
        send(x_ref.at[a], xs.at[FIRST, a], ag_send.at[0], ag_recv.at[0], right),
        send(x_ref.at[b], xs.at[FIRST, b], ag_send.at[1], ag_recv.at[1], left),
    ]
    tails = [
        send(xs.at[OWN, b], xs.at[SECOND, a], ag_send.at[2], ag_recv.at[2], right),
        send(xs.at[OWN, a], xs.at[SECOND, b], ag_send.at[3], ag_recv.at[3], left),
    ]
    onward = [
        send(xs.at[FIRST, a], xs.at[FAR, a], ag_send.at[4], ag_recv.at[4], right),
        send(xs.at[FIRST, b], xs.at[FAR, b], ag_send.at[5], ag_recv.at[5], left),
    ]
    direct = [
        send(to_dir.at[:, b], by_dir.at[:, b], dir_send.at[0], dir_recv.at[0], right),
        send(to_dir.at[:, a], by_dir.at[:, a], dir_send.at[1], dir_recv.at[1], left),
    ]

    def far(j):
        return (
            send(to_far.at[j, a], by_far.at[j, b], far_send.at[j, 0], far_recv.at[j, 0], right),
            send(to_far.at[j, b], by_far.at[j, a], far_send.at[j, 1], far_recv.at[j, 1], left),
        )

    def merged(j):
        return (
            send(to_mrg.at[j, b], by_mrg.at[j, a], mrg_send.at[j, 0], mrg_recv.at[j, 0], right),
            send(to_mrg.at[j, a], by_mrg.at[j, b], mrg_send.at[j, 1], mrg_recv.at[j, 1], left),
        )

    for copy in heads:
        copy.start()
    own_x.wait()
    for copy in tails:
        copy.start()

    for g in range(SLOTS_H):
        for copy in load_h(g):
            copy.start()
    for g in range(SLOTS_D):
        load_d(g).start()

    def hidden(p):
        @pl.loop(0, n_h)
        def _(i):
            g = p * n_h + i
            s = lax.rem(g, SLOTS_H)
            for copy in load_h(g):
                copy.wait()
            gate = jnp.dot(xs[p], wg[s], preferred_element_type=F32)
            up = jnp.dot(xs[p], wu[s], preferred_element_type=F32)
            col = pl.ds(pl.multiple_of(i * TILE_H, TILE_H), TILE_H)
            hid[:, col] = (jax.nn.gelu(gate) * up).astype(BF16)

            @pl.when(g + SLOTS_H < passes * n_h)
            def _():
                for copy in load_h(g + SLOTS_H):
                    copy.start()

    def down(p, put):
        @pl.loop(0, n_d)
        def _(j):
            g = p * n_d + j
            s = lax.rem(g, SLOTS_D)
            load_d(g).wait()
            put(j, jnp.dot(hid[...], wd[s], preferred_element_type=F32))

            @pl.when(g + SLOTS_D < passes * n_d)
            def _():
                load_d(g + SLOTS_D).start()

    def put_own(j, term):
        own[j] = term

    def put_direct(j, term):
        to_dir[j] = term.astype(BF16)

    def put_mid(j, term):
        mid[j] = term

    def put_far(j, term):
        to_far[j] = term.astype(BF16)
        for copy in far(j):
            copy.start()

    hidden(OWN)
    down(OWN, put_own)

    for copy in heads:
        copy.wait_recv()
    for copy in onward:
        copy.start()
    hidden(FIRST)
    down(FIRST, put_direct)
    for copy in direct:
        copy.start()

    for copy in tails:
        copy.wait_recv()
    hidden(SECOND)
    down(SECOND, put_mid)

    for copy in onward:
        copy.wait_recv()
    hidden(FAR)
    down(FAR, put_far)

    @pl.loop(0, n_d)
    def _(j):
        for copy in far(j):
            copy.wait_recv()
        to_mrg[j] = (mid[j] + by_far[j].astype(F32)).astype(BF16)
        for copy in merged(j):
            copy.start()

    for copy in direct:
        copy.wait_recv()
    for copy in heads + tails + onward + direct:
        copy.wait_send()

    @pl.loop(0, n_d)
    def _(j):
        for copy in far(j):
            copy.wait_send()

    last = n_d - 1
    own[last] += by_dir[last].astype(F32)

    @pl.loop(0, last)
    def _(j):
        for copy in merged(j):
            copy.wait_recv()
        col = pl.ds(pl.multiple_of(j * TILE_D, TILE_D), TILE_D)
        y_ref[:, col] = (own[j] + by_dir[j].astype(F32) + by_mrg[j].astype(F32)).astype(BF16)
        for copy in merged(j):
            copy.wait_send()

    for copy in merged(last):
        copy.wait_recv()
    for copy in merged(last):
        copy.wait_send()


def finish(y_ref, own, by_mrg, out_ref, piece, sem):
    last = own.shape[0] - 1
    copies = []
    for j in range(last + 1):
        col = pl.ds(j * TILE_D, TILE_D)
        if j == last:
            piece[...] = (own[j] + by_mrg[j].astype(F32)).astype(BF16)
        source = piece if j == last else y_ref.at[:, col]
        copies.append(pltpu.make_async_copy(source, out_ref.at[:, col], sem.at[j]))
        copies[-1].start()
    for copy in copies:
        copy.wait()


def solution(mesh):
    n = mesh.shape["tp"]

    def step(x, w_gate, w_up, w_down):
        rows, d = x.shape
        ff = w_gate.shape[1]
        n_d = d // TILE_D
        dma = pltpu.SemaphoreType.DMA
        pieces = (n_d, rows, TILE_D)
        vmem = pl.BlockSpec(memory_space=pltpu.VMEM)
        parts = pl.pallas_call(
            functools.partial(kernel, n),
            out_shape=(pltpu.VMEM((rows, d), BF16), pltpu.VMEM(pieces, F32), pltpu.VMEM(pieces, BF16)),
            in_specs=[pl.BlockSpec(memory_space=pl.ANY)] * 4,
            out_specs=(vmem, vmem, vmem),
            scratch_shapes=[
                pltpu.VMEM((n, rows, d), BF16),
                pltpu.VMEM((rows, ff), BF16),
                pltpu.VMEM((SLOTS_H, d, TILE_H), BF16),
                pltpu.VMEM((SLOTS_H, d, TILE_H), BF16),
                pltpu.VMEM((SLOTS_D, ff, TILE_D), BF16),
                pltpu.VMEM(pieces, F32),
                pltpu.VMEM(pieces, BF16),
                pltpu.VMEM(pieces, BF16),
                pltpu.VMEM(pieces, BF16),
                pltpu.VMEM(pieces, BF16),
                pltpu.VMEM(pieces, BF16),
                dma, dma((SLOTS_H,)), dma((SLOTS_H,)), dma((SLOTS_D,)),
                dma((6,)), dma((6,)), dma((2,)), dma((2,)),
                dma((n_d, 2)), dma((n_d, 2)), dma((n_d, 2)), dma((n_d, 2)),
            ],
            compiler_params=pltpu.CompilerParams(
                collective_id=0, has_side_effects=True, vmem_limit_bytes=VMEM_MIB * 1024 * 1024
            ),
            cost_estimate=pl.CostEstimate(
                flops=6 * n * rows * d * ff, bytes_accessed=6 * n * d * ff, transcendentals=n * rows * ff
            ),
            name="mlp_ring",
        )(x, w_gate, w_up, w_down)
        return pl.pallas_call(
            finish,
            out_shape=jax.ShapeDtypeStruct((rows, d), BF16),
            in_specs=[vmem] * 3,
            out_specs=pl.BlockSpec(memory_space=pl.ANY),
            scratch_shapes=[pltpu.VMEM((rows, TILE_D), BF16), dma((n_d,))],
            compiler_params=pltpu.CompilerParams(vmem_limit_bytes=FINISH_MIB * 1024 * 1024),
            name="finish",
        )(*parts)

    return jax.shard_map(
        step,
        mesh=mesh,
        in_specs=(P(("dp", "tp"), None), P(None, "tp"), P(None, "tp"), P("tp", None)),
        out_specs=P(("dp", "tp"), None),
        check_vma=False,
    )
```

```python
import functools

import jax
import jax.numpy as jnp
from jax import lax
from jax.experimental import pallas as pl
from jax.experimental.pallas import tpu as pltpu
from jax.sharding import PartitionSpec as P

MESH = pl.DeviceIdType.MESH
F32 = jnp.float32
BF16 = jnp.bfloat16

TILE_H = 256
TILE_D = 512
PIECE = 2
SLOTS_H = 3
SLOTS_D = 3
VMEM_MIB = 46
FINISH_MIB = 4

OWN, FIRST, SECOND, FAR = range(4)


def kernel(
    n,
    x_ref, wg_ref, wu_ref, wd_ref, y_ref, own, by_mrg,
    xs, hid, wg, wu, wd, mid, to_dir, to_far, to_mrg, by_dir, by_far,
    x_sem, wg_sem, wu_sem, wd_sem, ag_send, ag_recv, dir_send, dir_recv, far_send, far_recv, mrg_send, mrg_recv,
):
    me = lax.axis_index("tp")
    right, left = lax.rem(me + 1, n), lax.rem(me + n - 1, n)
    rows, d = x_ref.shape
    half = rows // 2
    n_h = wg_ref.shape[1] // TILE_H
    n_d = d // TILE_D
    n_p = n_d // PIECE
    passes = xs.shape[0]
    a, b = pl.ds(0, half), pl.ds(half, half)

    def load_h(g):
        col = pl.ds(pl.multiple_of(lax.rem(g, n_h) * TILE_H, TILE_H), TILE_H)
        s = lax.rem(g, SLOTS_H)
        return (
            pltpu.make_async_copy(wg_ref.at[:, col], wg.at[s], wg_sem.at[s]),
            pltpu.make_async_copy(wu_ref.at[:, col], wu.at[s], wu_sem.at[s]),
        )

    def load_d(g):
        col = pl.ds(pl.multiple_of(lax.rem(g, n_d) * TILE_D, TILE_D), TILE_D)
        s = lax.rem(g, SLOTS_D)
        return pltpu.make_async_copy(wd_ref.at[:, col], wd.at[s], wd_sem.at[s])

    def send(src, dst, send_sem, recv_sem, to):
        return pltpu.make_async_remote_copy(
            src_ref=src, dst_ref=dst, send_sem=send_sem, recv_sem=recv_sem, device_id={"tp": to}, device_id_type=MESH
        )

    barrier = pltpu.get_barrier_semaphore()
    for neighbour in (left, right):
        pl.semaphore_signal(barrier, inc=1, device_id={"tp": neighbour}, device_id_type=MESH)
    own_x = pltpu.make_async_copy(x_ref, xs.at[OWN], x_sem)
    own_x.start()
    pl.semaphore_wait(barrier, 2)

    heads = [
        send(x_ref.at[a], xs.at[FIRST, a], ag_send.at[0], ag_recv.at[0], right),
        send(x_ref.at[b], xs.at[FIRST, b], ag_send.at[1], ag_recv.at[1], left),
    ]
    tails = [
        send(xs.at[OWN, b], xs.at[SECOND, a], ag_send.at[2], ag_recv.at[2], right),
        send(xs.at[OWN, a], xs.at[SECOND, b], ag_send.at[3], ag_recv.at[3], left),
    ]
    onward = [
        send(xs.at[FIRST, a], xs.at[FAR, a], ag_send.at[4], ag_recv.at[4], right),
        send(xs.at[FIRST, b], xs.at[FAR, b], ag_send.at[5], ag_recv.at[5], left),
    ]
    direct = [
        send(to_dir.at[:, b], by_dir.at[:, b], dir_send.at[0], dir_recv.at[0], right),
        send(to_dir.at[:, a], by_dir.at[:, a], dir_send.at[1], dir_recv.at[1], left),
    ]

    def tiles(p):
        return pl.ds(p * PIECE, PIECE)

    def far(p):
        t = tiles(p)
        return (
            send(to_far.at[t, a], by_far.at[t, b], far_send.at[p, 0], far_recv.at[p, 0], right),
            send(to_far.at[t, b], by_far.at[t, a], far_send.at[p, 1], far_recv.at[p, 1], left),
        )

    def merged(p):
        t = tiles(p)
        return (
            send(to_mrg.at[t, b], by_mrg.at[t, a], mrg_send.at[p, 0], mrg_recv.at[p, 0], right),
            send(to_mrg.at[t, a], by_mrg.at[t, b], mrg_send.at[p, 1], mrg_recv.at[p, 1], left),
        )

    for copy in heads:
        copy.start()
    own_x.wait()
    for copy in tails:
        copy.start()

    for g in range(SLOTS_H):
        for copy in load_h(g):
            copy.start()
    for g in range(SLOTS_D):
        load_d(g).start()

    def hidden(p):
        @pl.loop(0, n_h)
        def _(i):
            g = p * n_h + i
            s = lax.rem(g, SLOTS_H)
            for copy in load_h(g):
                copy.wait()
            gate = jnp.dot(xs[p], wg[s], preferred_element_type=F32)
            up = jnp.dot(xs[p], wu[s], preferred_element_type=F32)
            col = pl.ds(pl.multiple_of(i * TILE_H, TILE_H), TILE_H)
            hid[:, col] = (jax.nn.gelu(gate) * up).astype(BF16)

            @pl.when(g + SLOTS_H < passes * n_h)
            def _():
                for copy in load_h(g + SLOTS_H):
                    copy.start()

    def down(p, put):
        @pl.loop(0, n_d)
        def _(j):
            g = p * n_d + j
            s = lax.rem(g, SLOTS_D)
            load_d(g).wait()
            put(j, jnp.dot(hid[...], wd[s], preferred_element_type=F32))

            @pl.when(g + SLOTS_D < passes * n_d)
            def _():
                load_d(g + SLOTS_D).start()

    def put_own(j, term):
        own[j] = term

    def put_direct(j, term):
        to_dir[j] = term.astype(BF16)

    def put_mid(j, term):
        mid[j] = term

    def put_far(j, term):
        to_far[j] = term.astype(BF16)

        @pl.when(lax.rem(j, PIECE) == PIECE - 1)
        def _():
            for copy in far(lax.div(j, PIECE)):
                copy.start()

    hidden(OWN)
    down(OWN, put_own)

    for copy in heads:
        copy.wait_recv()
    for copy in onward:
        copy.start()
    hidden(FIRST)
    down(FIRST, put_direct)
    for copy in direct:
        copy.start()

    for copy in tails:
        copy.wait_recv()
    hidden(SECOND)
    down(SECOND, put_mid)

    for copy in onward:
        copy.wait_recv()
    hidden(FAR)
    down(FAR, put_far)

    @pl.loop(0, n_p)
    def _(p):
        for copy in far(p):
            copy.wait_recv()

        @pl.loop(0, PIECE)
        def _(k):
            j = p * PIECE + k
            to_mrg[j] = (mid[j] + by_far[j].astype(F32)).astype(BF16)

        for copy in merged(p):
            copy.start()

    for copy in direct:
        copy.wait_recv()
    for copy in heads + tails + onward + direct:
        copy.wait_send()

    @pl.loop(0, n_p)
    def _(p):
        for copy in far(p):
            copy.wait_send()

    last = n_p - 1

    @pl.loop(last * PIECE, n_d)
    def _(j):
        own[j] += by_dir[j].astype(F32)

    @pl.loop(0, last)
    def _(p):
        for copy in merged(p):
            copy.wait_recv()

        @pl.loop(0, PIECE)
        def _(k):
            j = p * PIECE + k
            col = pl.ds(pl.multiple_of(j * TILE_D, TILE_D), TILE_D)
            y_ref[:, col] = (own[j] + by_dir[j].astype(F32) + by_mrg[j].astype(F32)).astype(BF16)

        for copy in merged(p):
            copy.wait_send()

    for copy in merged(last):
        copy.wait_recv()
    for copy in merged(last):
        copy.wait_send()


def finish(y_ref, own, by_mrg, out_ref, piece, sem):
    n_d = own.shape[0]
    done = n_d - PIECE
    col = pl.ds(0, done * TILE_D)
    copies = [pltpu.make_async_copy(y_ref.at[:, col], out_ref.at[:, col], sem.at[PIECE])]
    copies[0].start()
    for k in range(PIECE):
        j = done + k
        piece[k] = (own[j] + by_mrg[j].astype(F32)).astype(BF16)
        copies.append(pltpu.make_async_copy(piece.at[k], out_ref.at[:, pl.ds(j * TILE_D, TILE_D)], sem.at[k]))
        copies[-1].start()
    for copy in copies:
        copy.wait()


def solution(mesh):
    n = mesh.shape["tp"]

    def step(x, w_gate, w_up, w_down):
        rows, d = x.shape
        ff = w_gate.shape[1]
        n_d = d // TILE_D
        n_p = n_d // PIECE
        dma = pltpu.SemaphoreType.DMA
        pieces = (n_d, rows, TILE_D)
        vmem = pl.BlockSpec(memory_space=pltpu.VMEM)
        parts = pl.pallas_call(
            functools.partial(kernel, n),
            out_shape=(pltpu.VMEM((rows, d), BF16), pltpu.VMEM(pieces, F32), pltpu.VMEM(pieces, BF16)),
            in_specs=[pl.BlockSpec(memory_space=pl.ANY)] * 4,
            out_specs=(vmem, vmem, vmem),
            scratch_shapes=[
                pltpu.VMEM((n, rows, d), BF16),
                pltpu.VMEM((rows, ff), BF16),
                pltpu.VMEM((SLOTS_H, d, TILE_H), BF16),
                pltpu.VMEM((SLOTS_H, d, TILE_H), BF16),
                pltpu.VMEM((SLOTS_D, ff, TILE_D), BF16),
                pltpu.VMEM(pieces, F32),
                pltpu.VMEM(pieces, BF16),
                pltpu.VMEM(pieces, BF16),
                pltpu.VMEM(pieces, BF16),
                pltpu.VMEM(pieces, BF16),
                pltpu.VMEM(pieces, BF16),
                dma, dma((SLOTS_H,)), dma((SLOTS_H,)), dma((SLOTS_D,)),
                dma((6,)), dma((6,)), dma((2,)), dma((2,)),
                dma((n_p, 2)), dma((n_p, 2)), dma((n_p, 2)), dma((n_p, 2)),
            ],
            compiler_params=pltpu.CompilerParams(
                collective_id=0, has_side_effects=True, vmem_limit_bytes=VMEM_MIB * 1024 * 1024
            ),
            cost_estimate=pl.CostEstimate(
                flops=6 * n * rows * d * ff, bytes_accessed=6 * n * d * ff, transcendentals=n * rows * ff
            ),
            name="mlp_ring",
        )(x, w_gate, w_up, w_down)
        return pl.pallas_call(
            finish,
            out_shape=jax.ShapeDtypeStruct((rows, d), BF16),
            in_specs=[vmem] * 3,
            out_specs=pl.BlockSpec(memory_space=pl.ANY),
            scratch_shapes=[pltpu.VMEM((PIECE, rows, TILE_D), BF16), dma((PIECE + 1,))],
            compiler_params=pltpu.CompilerParams(vmem_limit_bytes=FINISH_MIB * 1024 * 1024),
            name="finish",
        )(*parts)

    return jax.shard_map(
        step,
        mesh=mesh,
        in_specs=(P(("dp", "tp"), None), P(None, "tp"), P(None, "tp"), P("tp", None)),
        out_specs=P(("dp", "tp"), None),
        check_vma=False,
    )
```

```python
import functools

import jax
import jax.numpy as jnp
from jax import lax
from jax.experimental import pallas as pl
from jax.experimental.pallas import tpu as pltpu
from jax.sharding import PartitionSpec as P

MESH = pl.DeviceIdType.MESH
F32 = jnp.float32
BF16 = jnp.bfloat16

TILE_H = 256
TILE_D = 512
PIECE = 4
SLOTS_H = 3
SLOTS_D = 3
VMEM_MIB = 46
FINISH_MIB = 4

OWN, FIRST, SECOND, FAR = range(4)


def kernel(
    n,
    x_ref, wg_ref, wu_ref, wd_ref, y_ref, own, by_mrg,
    xs, hid, wg, wu, wd, mid, to_dir, to_far, to_mrg, by_dir, by_far,
    x_sem, wg_sem, wu_sem, wd_sem, ag_send, ag_recv, dir_send, dir_recv, far_send, far_recv, mrg_send, mrg_recv,
):
    me = lax.axis_index("tp")
    right, left = lax.rem(me + 1, n), lax.rem(me + n - 1, n)
    rows, d = x_ref.shape
    half = rows // 2
    n_h = wg_ref.shape[1] // TILE_H
    n_d = d // TILE_D
    n_p = n_d // PIECE
    passes = xs.shape[0]
    a, b = pl.ds(0, half), pl.ds(half, half)

    def load_h(g):
        col = pl.ds(pl.multiple_of(lax.rem(g, n_h) * TILE_H, TILE_H), TILE_H)
        s = lax.rem(g, SLOTS_H)
        return (
            pltpu.make_async_copy(wg_ref.at[:, col], wg.at[s], wg_sem.at[s]),
            pltpu.make_async_copy(wu_ref.at[:, col], wu.at[s], wu_sem.at[s]),
        )

    def load_d(g):
        col = pl.ds(pl.multiple_of(lax.rem(g, n_d) * TILE_D, TILE_D), TILE_D)
        s = lax.rem(g, SLOTS_D)
        return pltpu.make_async_copy(wd_ref.at[:, col], wd.at[s], wd_sem.at[s])

    def send(src, dst, send_sem, recv_sem, to):
        return pltpu.make_async_remote_copy(
            src_ref=src, dst_ref=dst, send_sem=send_sem, recv_sem=recv_sem, device_id={"tp": to}, device_id_type=MESH
        )

    barrier = pltpu.get_barrier_semaphore()
    for neighbour in (left, right):
        pl.semaphore_signal(barrier, inc=1, device_id={"tp": neighbour}, device_id_type=MESH)
    own_x = pltpu.make_async_copy(x_ref, xs.at[OWN], x_sem)
    own_x.start()
    pl.semaphore_wait(barrier, 2)

    heads = [
        send(x_ref.at[a], xs.at[FIRST, a], ag_send.at[0], ag_recv.at[0], right),
        send(x_ref.at[b], xs.at[FIRST, b], ag_send.at[1], ag_recv.at[1], left),
    ]
    tails = [
        send(xs.at[OWN, b], xs.at[SECOND, a], ag_send.at[2], ag_recv.at[2], right),
        send(xs.at[OWN, a], xs.at[SECOND, b], ag_send.at[3], ag_recv.at[3], left),
    ]
    onward = [
        send(xs.at[FIRST, a], xs.at[FAR, a], ag_send.at[4], ag_recv.at[4], right),
        send(xs.at[FIRST, b], xs.at[FAR, b], ag_send.at[5], ag_recv.at[5], left),
    ]
    direct = [
        send(to_dir.at[:, b], by_dir.at[:, b], dir_send.at[0], dir_recv.at[0], right),
        send(to_dir.at[:, a], by_dir.at[:, a], dir_send.at[1], dir_recv.at[1], left),
    ]

    def tiles(p):
        return pl.ds(p * PIECE, PIECE)

    def far(p):
        t = tiles(p)
        return (
            send(to_far.at[t, a], by_far.at[t, b], far_send.at[p, 0], far_recv.at[p, 0], right),
            send(to_far.at[t, b], by_far.at[t, a], far_send.at[p, 1], far_recv.at[p, 1], left),
        )

    def merged(p):
        t = tiles(p)
        return (
            send(to_mrg.at[t, b], by_mrg.at[t, a], mrg_send.at[p, 0], mrg_recv.at[p, 0], right),
            send(to_mrg.at[t, a], by_mrg.at[t, b], mrg_send.at[p, 1], mrg_recv.at[p, 1], left),
        )

    for copy in heads:
        copy.start()
    own_x.wait()
    for copy in tails:
        copy.start()

    for g in range(SLOTS_H):
        for copy in load_h(g):
            copy.start()
    for g in range(SLOTS_D):
        load_d(g).start()

    def hidden(p):
        @pl.loop(0, n_h)
        def _(i):
            g = p * n_h + i
            s = lax.rem(g, SLOTS_H)
            for copy in load_h(g):
                copy.wait()
            gate = jnp.dot(xs[p], wg[s], preferred_element_type=F32)
            up = jnp.dot(xs[p], wu[s], preferred_element_type=F32)
            col = pl.ds(pl.multiple_of(i * TILE_H, TILE_H), TILE_H)
            hid[:, col] = (jax.nn.gelu(gate) * up).astype(BF16)

            @pl.when(g + SLOTS_H < passes * n_h)
            def _():
                for copy in load_h(g + SLOTS_H):
                    copy.start()

    def down(p, put):
        @pl.loop(0, n_d)
        def _(j):
            g = p * n_d + j
            s = lax.rem(g, SLOTS_D)
            load_d(g).wait()
            put(j, jnp.dot(hid[...], wd[s], preferred_element_type=F32))

            @pl.when(g + SLOTS_D < passes * n_d)
            def _():
                load_d(g + SLOTS_D).start()

    def put_own(j, term):
        own[j] = term

    def put_direct(j, term):
        to_dir[j] = term.astype(BF16)

    def put_mid(j, term):
        mid[j] = term

    def put_far(j, term):
        to_far[j] = term.astype(BF16)

        @pl.when(lax.rem(j, PIECE) == PIECE - 1)
        def _():
            for copy in far(lax.div(j, PIECE)):
                copy.start()

    hidden(OWN)
    down(OWN, put_own)

    for copy in heads:
        copy.wait_recv()
    for copy in onward:
        copy.start()
    hidden(FIRST)
    down(FIRST, put_direct)
    for copy in direct:
        copy.start()

    for copy in tails:
        copy.wait_recv()
    hidden(SECOND)
    down(SECOND, put_mid)

    for copy in onward:
        copy.wait_recv()
    hidden(FAR)
    down(FAR, put_far)

    @pl.loop(0, n_p)
    def _(p):
        for copy in far(p):
            copy.wait_recv()

        @pl.loop(0, PIECE)
        def _(k):
            j = p * PIECE + k
            to_mrg[j] = (mid[j] + by_far[j].astype(F32)).astype(BF16)

        for copy in merged(p):
            copy.start()

    for copy in direct:
        copy.wait_recv()
    for copy in heads + tails + onward + direct:
        copy.wait_send()

    @pl.loop(0, n_p)
    def _(p):
        for copy in far(p):
            copy.wait_send()

    last = n_p - 1

    @pl.loop(last * PIECE, n_d)
    def _(j):
        own[j] += by_dir[j].astype(F32)

    @pl.loop(0, last)
    def _(p):
        for copy in merged(p):
            copy.wait_recv()

        @pl.loop(0, PIECE)
        def _(k):
            j = p * PIECE + k
            col = pl.ds(pl.multiple_of(j * TILE_D, TILE_D), TILE_D)
            y_ref[:, col] = (own[j] + by_dir[j].astype(F32) + by_mrg[j].astype(F32)).astype(BF16)

        for copy in merged(p):
            copy.wait_send()

    for copy in merged(last):
        copy.wait_recv()
    for copy in merged(last):
        copy.wait_send()


def finish(y_ref, own, by_mrg, out_ref, piece, sem):
    n_d = own.shape[0]
    done = n_d - PIECE
    col = pl.ds(0, done * TILE_D)
    copies = [pltpu.make_async_copy(y_ref.at[:, col], out_ref.at[:, col], sem.at[PIECE])]
    copies[0].start()
    for k in range(PIECE):
        j = done + k
        piece[k] = (own[j] + by_mrg[j].astype(F32)).astype(BF16)
        copies.append(pltpu.make_async_copy(piece.at[k], out_ref.at[:, pl.ds(j * TILE_D, TILE_D)], sem.at[k]))
        copies[-1].start()
    for copy in copies:
        copy.wait()


def solution(mesh):
    n = mesh.shape["tp"]

    def step(x, w_gate, w_up, w_down):
        rows, d = x.shape
        ff = w_gate.shape[1]
        n_d = d // TILE_D
        n_p = n_d // PIECE
        dma = pltpu.SemaphoreType.DMA
        pieces = (n_d, rows, TILE_D)
        vmem = pl.BlockSpec(memory_space=pltpu.VMEM)
        parts = pl.pallas_call(
            functools.partial(kernel, n),
            out_shape=(pltpu.VMEM((rows, d), BF16), pltpu.VMEM(pieces, F32), pltpu.VMEM(pieces, BF16)),
            in_specs=[pl.BlockSpec(memory_space=pl.ANY)] * 4,
            out_specs=(vmem, vmem, vmem),
            scratch_shapes=[
                pltpu.VMEM((n, rows, d), BF16),
                pltpu.VMEM((rows, ff), BF16),
                pltpu.VMEM((SLOTS_H, d, TILE_H), BF16),
                pltpu.VMEM((SLOTS_H, d, TILE_H), BF16),
                pltpu.VMEM((SLOTS_D, ff, TILE_D), BF16),
                pltpu.VMEM(pieces, F32),
                pltpu.VMEM(pieces, BF16),
                pltpu.VMEM(pieces, BF16),
                pltpu.VMEM(pieces, BF16),
                pltpu.VMEM(pieces, BF16),
                pltpu.VMEM(pieces, BF16),
                dma, dma((SLOTS_H,)), dma((SLOTS_H,)), dma((SLOTS_D,)),
                dma((6,)), dma((6,)), dma((2,)), dma((2,)),
                dma((n_p, 2)), dma((n_p, 2)), dma((n_p, 2)), dma((n_p, 2)),
            ],
            compiler_params=pltpu.CompilerParams(
                collective_id=0, has_side_effects=True, vmem_limit_bytes=VMEM_MIB * 1024 * 1024
            ),
            cost_estimate=pl.CostEstimate(
                flops=6 * n * rows * d * ff, bytes_accessed=6 * n * d * ff, transcendentals=n * rows * ff
            ),
            name="mlp_ring",
        )(x, w_gate, w_up, w_down)
        return pl.pallas_call(
            finish,
            out_shape=jax.ShapeDtypeStruct((rows, d), BF16),
            in_specs=[vmem] * 3,
            out_specs=pl.BlockSpec(memory_space=pl.ANY),
            scratch_shapes=[pltpu.VMEM((PIECE, rows, TILE_D), BF16), dma((PIECE + 1,))],
            compiler_params=pltpu.CompilerParams(vmem_limit_bytes=FINISH_MIB * 1024 * 1024),
            name="finish",
        )(*parts)

    return jax.shard_map(
        step,
        mesh=mesh,
        in_specs=(P(("dp", "tp"), None), P(None, "tp"), P(None, "tp"), P("tp", None)),
        out_specs=P(("dp", "tp"), None),
        check_vma=False,
    )
```

```python
import functools

import jax
import jax.numpy as jnp
from jax import lax
from jax.experimental import pallas as pl
from jax.experimental.pallas import tpu as pltpu
from jax.sharding import PartitionSpec as P

MESH = pl.DeviceIdType.MESH
F32 = jnp.float32
BF16 = jnp.bfloat16

TILE_H = 256
TILE_D = 512
BACK = 2
SLOTS_H = 3
SLOTS_D = 3
VMEM_MIB = 48
FINISH_MIB = 4

OWN, FIRST, SECOND, FAR = range(4)


def kernel(
    n,
    x_ref, wg_ref, wu_ref, wd_ref, y_ref, own, by_mrg,
    xs, hid, wg, wu, wd, mid, to_dir, to_far, to_mrg, by_dir, by_far,
    x_sem, wg_sem, wu_sem, wd_sem, ag_send, ag_recv, dir_send, dir_recv, far_send, far_recv, mrg_send, mrg_recv,
):
    me = lax.axis_index("tp")
    right, left = lax.rem(me + 1, n), lax.rem(me + n - 1, n)
    rows, d = x_ref.shape
    half = rows // 2
    n_h = wg_ref.shape[1] // TILE_H
    n_d = d // TILE_D
    pieces = ((0, n_d - BACK), (n_d - BACK, n_d))
    passes = xs.shape[0]
    a, b = pl.ds(0, half), pl.ds(half, half)

    def load_h(g):
        col = pl.ds(pl.multiple_of(lax.rem(g, n_h) * TILE_H, TILE_H), TILE_H)
        s = lax.rem(g, SLOTS_H)
        return (
            pltpu.make_async_copy(wg_ref.at[:, col], wg.at[s], wg_sem.at[s]),
            pltpu.make_async_copy(wu_ref.at[:, col], wu.at[s], wu_sem.at[s]),
        )

    def load_d(g):
        col = pl.ds(pl.multiple_of(lax.rem(g, n_d) * TILE_D, TILE_D), TILE_D)
        s = lax.rem(g, SLOTS_D)
        return pltpu.make_async_copy(wd_ref.at[:, col], wd.at[s], wd_sem.at[s])

    def send(src, dst, send_sem, recv_sem, to):
        return pltpu.make_async_remote_copy(
            src_ref=src, dst_ref=dst, send_sem=send_sem, recv_sem=recv_sem, device_id={"tp": to}, device_id_type=MESH
        )

    barrier = pltpu.get_barrier_semaphore()
    for neighbour in (left, right):
        pl.semaphore_signal(barrier, inc=1, device_id={"tp": neighbour}, device_id_type=MESH)
    own_x = pltpu.make_async_copy(x_ref, xs.at[OWN], x_sem)
    own_x.start()
    pl.semaphore_wait(barrier, 2)

    heads = [
        send(x_ref.at[a], xs.at[FIRST, a], ag_send.at[0], ag_recv.at[0], right),
        send(x_ref.at[b], xs.at[FIRST, b], ag_send.at[1], ag_recv.at[1], left),
    ]
    tails = [
        send(xs.at[OWN, b], xs.at[SECOND, a], ag_send.at[2], ag_recv.at[2], right),
        send(xs.at[OWN, a], xs.at[SECOND, b], ag_send.at[3], ag_recv.at[3], left),
    ]
    onward = [
        send(xs.at[FIRST, a], xs.at[FAR, a], ag_send.at[4], ag_recv.at[4], right),
        send(xs.at[FIRST, b], xs.at[FAR, b], ag_send.at[5], ag_recv.at[5], left),
    ]
    direct = [
        send(to_dir.at[:, b], by_dir.at[:, b], dir_send.at[0], dir_recv.at[0], right),
        send(to_dir.at[:, a], by_dir.at[:, a], dir_send.at[1], dir_recv.at[1], left),
    ]

    def far(p):
        t = pl.ds(pieces[p][0], pieces[p][1] - pieces[p][0])
        return (
            send(to_far.at[t, a], by_far.at[t, b], far_send.at[p, 0], far_recv.at[p, 0], right),
            send(to_far.at[t, b], by_far.at[t, a], far_send.at[p, 1], far_recv.at[p, 1], left),
        )

    def merged(p):
        t = pl.ds(pieces[p][0], pieces[p][1] - pieces[p][0])
        return (
            send(to_mrg.at[t, b], by_mrg.at[t, a], mrg_send.at[p, 0], mrg_recv.at[p, 0], right),
            send(to_mrg.at[t, a], by_mrg.at[t, b], mrg_send.at[p, 1], mrg_recv.at[p, 1], left),
        )

    for copy in heads:
        copy.start()
    own_x.wait()
    for copy in tails:
        copy.start()

    for g in range(SLOTS_H):
        for copy in load_h(g):
            copy.start()
    for g in range(SLOTS_D):
        load_d(g).start()

    def hidden(p):
        @pl.loop(0, n_h)
        def _(i):
            g = p * n_h + i
            s = lax.rem(g, SLOTS_H)
            for copy in load_h(g):
                copy.wait()
            gate = jnp.dot(xs[p], wg[s], preferred_element_type=F32)
            up = jnp.dot(xs[p], wu[s], preferred_element_type=F32)
            col = pl.ds(pl.multiple_of(i * TILE_H, TILE_H), TILE_H)
            hid[min(p, 1), :, col] = (jax.nn.gelu(gate) * up).astype(BF16)

            @pl.when(g + SLOTS_H < passes * n_h)
            def _():
                for copy in load_h(g + SLOTS_H):
                    copy.start()

    def down(turn, p, put):
        @pl.loop(0, n_d)
        def _(j):
            g = turn * n_d + j
            s = lax.rem(g, SLOTS_D)
            load_d(g).wait()
            put(j, jnp.dot(hid[min(p, 1)], wd[s], preferred_element_type=F32))

            @pl.when(g + SLOTS_D < passes * n_d)
            def _():
                load_d(g + SLOTS_D).start()

    def put_own(j, term):
        own[j] = term

    def put_direct(j, term):
        to_dir[j] = term.astype(BF16)

    def put_mid(j, term):
        mid[j] = term

    def put_far(j, term):
        to_far[j] = term.astype(BF16)

        for p, (_, end) in enumerate(pieces):

            @pl.when(j == end - 1)
            def _():
                for copy in far(p):
                    copy.start()

    hidden(OWN)

    for copy in heads:
        copy.wait_recv()
    for copy in onward:
        copy.start()
    hidden(FIRST)
    down(0, FIRST, put_direct)
    for copy in direct:
        copy.start()

    for copy in tails:
        copy.wait_recv()
    hidden(SECOND)
    down(1, SECOND, put_mid)

    for copy in onward:
        copy.wait_recv()
    hidden(FAR)
    down(2, FAR, put_far)
    down(3, OWN, put_own)

    for p, (start, end) in enumerate(pieces):
        for copy in far(p):
            copy.wait_recv()

        @pl.loop(start, end)
        def _(j):
            to_mrg[j] = (mid[j] + by_far[j].astype(F32)).astype(BF16)

        for copy in merged(p):
            copy.start()

    for copy in direct:
        copy.wait_recv()

    @pl.loop(0, n_d)
    def _(j):
        own[j] += by_dir[j].astype(F32)

    for copy in heads + tails + onward + [*direct, *far(0), *far(1)]:
        copy.wait_send()
    for copy in merged(0):
        copy.wait_recv()

    @pl.loop(*pieces[0])
    def _(j):
        col = pl.ds(pl.multiple_of(j * TILE_D, TILE_D), TILE_D)
        y_ref[:, col] = (own[j] + by_mrg[j].astype(F32)).astype(BF16)

    for copy in merged(0):
        copy.wait_send()
    for copy in merged(1):
        copy.wait_recv()
    for copy in merged(1):
        copy.wait_send()


def finish(y_ref, own, by_mrg, out_ref, piece, sem):
    done = own.shape[0] - BACK
    col = pl.ds(0, done * TILE_D)
    copies = [pltpu.make_async_copy(y_ref.at[:, col], out_ref.at[:, col], sem.at[BACK])]
    copies[0].start()
    for k in range(BACK):
        j = done + k
        piece[k] = (own[j] + by_mrg[j].astype(F32)).astype(BF16)
        copies.append(pltpu.make_async_copy(piece.at[k], out_ref.at[:, pl.ds(j * TILE_D, TILE_D)], sem.at[k]))
        copies[-1].start()
    for copy in copies:
        copy.wait()


def solution(mesh):
    n = mesh.shape["tp"]

    def step(x, w_gate, w_up, w_down):
        rows, d = x.shape
        ff = w_gate.shape[1]
        n_d = d // TILE_D
        dma = pltpu.SemaphoreType.DMA
        pieces = (n_d, rows, TILE_D)
        vmem = pl.BlockSpec(memory_space=pltpu.VMEM)
        parts = pl.pallas_call(
            functools.partial(kernel, n),
            out_shape=(pltpu.VMEM((rows, d), BF16), pltpu.VMEM(pieces, F32), pltpu.VMEM(pieces, BF16)),
            in_specs=[pl.BlockSpec(memory_space=pl.ANY)] * 4,
            out_specs=(vmem, vmem, vmem),
            scratch_shapes=[
                pltpu.VMEM((n, rows, d), BF16),
                pltpu.VMEM((2, rows, ff), BF16),
                pltpu.VMEM((SLOTS_H, d, TILE_H), BF16),
                pltpu.VMEM((SLOTS_H, d, TILE_H), BF16),
                pltpu.VMEM((SLOTS_D, ff, TILE_D), BF16),
                pltpu.VMEM(pieces, F32),
                pltpu.VMEM(pieces, BF16),
                pltpu.VMEM(pieces, BF16),
                pltpu.VMEM(pieces, BF16),
                pltpu.VMEM(pieces, BF16),
                pltpu.VMEM(pieces, BF16),
                dma, dma((SLOTS_H,)), dma((SLOTS_H,)), dma((SLOTS_D,)),
                dma((6,)), dma((6,)), dma((2,)), dma((2,)),
                dma((2, 2)), dma((2, 2)), dma((2, 2)), dma((2, 2)),
            ],
            compiler_params=pltpu.CompilerParams(
                collective_id=0, has_side_effects=True, vmem_limit_bytes=VMEM_MIB * 1024 * 1024
            ),
            cost_estimate=pl.CostEstimate(
                flops=6 * n * rows * d * ff, bytes_accessed=6 * n * d * ff, transcendentals=n * rows * ff
            ),
            name="mlp_ring",
        )(x, w_gate, w_up, w_down)
        return pl.pallas_call(
            finish,
            out_shape=jax.ShapeDtypeStruct((rows, d), BF16),
            in_specs=[vmem] * 3,
            out_specs=pl.BlockSpec(memory_space=pl.ANY),
            scratch_shapes=[pltpu.VMEM((BACK, rows, TILE_D), BF16), dma((BACK + 1,))],
            compiler_params=pltpu.CompilerParams(vmem_limit_bytes=FINISH_MIB * 1024 * 1024),
            name="finish",
        )(*parts)

    return jax.shard_map(
        step,
        mesh=mesh,
        in_specs=(P(("dp", "tp"), None), P(None, "tp"), P(None, "tp"), P("tp", None)),
        out_specs=P(("dp", "tp"), None),
        check_vma=False,
    )
```

```python
import functools

import jax
import jax.numpy as jnp
from jax import lax
from jax.experimental import pallas as pl
from jax.experimental.pallas import tpu as pltpu
from jax.sharding import PartitionSpec as P

MESH = pl.DeviceIdType.MESH
F32 = jnp.float32
BF16 = jnp.bfloat16

TILE_H = 256
TILE_D = 512
BACK = 2
SLOTS_H = 3
SLOTS_D = 3
VMEM_MIB = 48
FINISH_MIB = 4

OWN, FIRST, SECOND, FAR = range(4)


def kernel(
    n,
    x_ref, wg_ref, wu_ref, wd_ref, y_ref, own, by_mrg,
    xs, hid, wg, wu, wd, mid, to_dir, to_far, to_mrg, by_dir, by_far,
    x_sem, wg_sem, wu_sem, wd_sem, ag_send, ag_recv, dir_send, dir_recv, far_send, far_recv, mrg_send, mrg_recv,
):
    me = lax.axis_index("tp")
    right, left = lax.rem(me + 1, n), lax.rem(me + n - 1, n)
    rows, d = x_ref.shape
    half = rows // 2
    n_h = wg_ref.shape[1] // TILE_H
    n_d = d // TILE_D
    pieces = ((0, n_d - BACK), (n_d - BACK, n_d))
    passes = xs.shape[0]
    a, b = pl.ds(0, half), pl.ds(half, half)

    def load_h(g):
        col = pl.ds(pl.multiple_of(lax.rem(g, n_h) * TILE_H, TILE_H), TILE_H)
        s = lax.rem(g, SLOTS_H)
        return (
            pltpu.make_async_copy(wg_ref.at[:, col], wg.at[s], wg_sem.at[s]),
            pltpu.make_async_copy(wu_ref.at[:, col], wu.at[s], wu_sem.at[s]),
        )

    def load_d(g):
        col = pl.ds(pl.multiple_of(lax.rem(g, n_d) * TILE_D, TILE_D), TILE_D)
        s = lax.rem(g, SLOTS_D)
        return pltpu.make_async_copy(wd_ref.at[:, col], wd.at[s], wd_sem.at[s])

    def send(src, dst, send_sem, recv_sem, to):
        return pltpu.make_async_remote_copy(
            src_ref=src, dst_ref=dst, send_sem=send_sem, recv_sem=recv_sem, device_id={"tp": to}, device_id_type=MESH
        )

    barrier = pltpu.get_barrier_semaphore()
    for neighbour in (left, right):
        pl.semaphore_signal(barrier, inc=1, device_id={"tp": neighbour}, device_id_type=MESH)
    own_x = [pltpu.make_async_copy(x_ref.at[h], xs.at[OWN, h], x_sem.at[k]) for k, h in enumerate((b, a))]
    for copy in own_x:
        copy.start()
    pl.semaphore_wait(barrier, 2)

    heads = [
        send(x_ref.at[a], xs.at[FIRST, a], ag_send.at[0], ag_recv.at[0], right),
        send(xs.at[OWN, b], xs.at[FIRST, b], ag_send.at[1], ag_recv.at[1], left),
    ]
    tails = [
        send(xs.at[OWN, b], xs.at[SECOND, a], ag_send.at[2], ag_recv.at[2], right),
        send(xs.at[OWN, a], xs.at[SECOND, b], ag_send.at[3], ag_recv.at[3], left),
    ]
    onward = [
        send(xs.at[FIRST, a], xs.at[FAR, a], ag_send.at[4], ag_recv.at[4], right),
        send(xs.at[FIRST, b], xs.at[FAR, b], ag_send.at[5], ag_recv.at[5], left),
    ]
    direct = [
        send(to_dir.at[:, b], by_dir.at[:, b], dir_send.at[0], dir_recv.at[0], right),
        send(to_dir.at[:, a], by_dir.at[:, a], dir_send.at[1], dir_recv.at[1], left),
    ]

    def far(p):
        t = pl.ds(pieces[p][0], pieces[p][1] - pieces[p][0])
        return (
            send(to_far.at[t, a], by_far.at[t, b], far_send.at[p, 0], far_recv.at[p, 0], right),
            send(to_far.at[t, b], by_far.at[t, a], far_send.at[p, 1], far_recv.at[p, 1], left),
        )

    def merged(p):
        t = pl.ds(pieces[p][0], pieces[p][1] - pieces[p][0])
        return (
            send(to_mrg.at[t, b], by_mrg.at[t, a], mrg_send.at[p, 0], mrg_recv.at[p, 0], right),
            send(to_mrg.at[t, a], by_mrg.at[t, b], mrg_send.at[p, 1], mrg_recv.at[p, 1], left),
        )

    heads[0].start()
    own_x[0].wait()
    heads[1].start()
    own_x[1].wait()
    for copy in tails:
        copy.start()

    for g in range(SLOTS_H):
        for copy in load_h(g):
            copy.start()
    for g in range(SLOTS_D):
        load_d(g).start()

    def hidden(p):
        @pl.loop(0, n_h)
        def _(i):
            g = p * n_h + i
            s = lax.rem(g, SLOTS_H)
            for copy in load_h(g):
                copy.wait()
            gate = jnp.dot(xs[p], wg[s], preferred_element_type=F32)
            up = jnp.dot(xs[p], wu[s], preferred_element_type=F32)
            col = pl.ds(pl.multiple_of(i * TILE_H, TILE_H), TILE_H)
            hid[min(p, 1), :, col] = (jax.nn.gelu(gate) * up).astype(BF16)

            @pl.when(g + SLOTS_H < passes * n_h)
            def _():
                for copy in load_h(g + SLOTS_H):
                    copy.start()

    def down(turn, p, put):
        @pl.loop(0, n_d)
        def _(j):
            g = turn * n_d + j
            s = lax.rem(g, SLOTS_D)
            load_d(g).wait()
            put(j, jnp.dot(hid[min(p, 1)], wd[s], preferred_element_type=F32))

            @pl.when(g + SLOTS_D < passes * n_d)
            def _():
                load_d(g + SLOTS_D).start()

    def put_own(j, term):
        own[j] = term

    def put_direct(j, term):
        to_dir[j] = term.astype(BF16)

    def put_mid(j, term):
        mid[j] = term

    def put_far(j, term):
        to_far[j] = term.astype(BF16)

        for p, (_, end) in enumerate(pieces):

            @pl.when(j == end - 1)
            def _():
                for copy in far(p):
                    copy.start()

    hidden(OWN)

    for copy in heads:
        copy.wait_recv()
    for copy in onward:
        copy.start()
    hidden(FIRST)
    down(0, FIRST, put_direct)
    for copy in direct:
        copy.start()

    for copy in tails:
        copy.wait_recv()
    hidden(SECOND)
    down(1, SECOND, put_mid)

    for copy in onward:
        copy.wait_recv()
    hidden(FAR)
    down(2, FAR, put_far)
    down(3, OWN, put_own)

    for p, (start, end) in enumerate(pieces):
        for copy in far(p):
            copy.wait_recv()

        @pl.loop(start, end)
        def _(j):
            to_mrg[j] = (mid[j] + by_far[j].astype(F32)).astype(BF16)

        for copy in merged(p):
            copy.start()

    for copy in direct:
        copy.wait_recv()

    @pl.loop(0, n_d)
    def _(j):
        own[j] += by_dir[j].astype(F32)

    for copy in heads + tails + onward + [*direct, *far(0), *far(1)]:
        copy.wait_send()
    for copy in merged(0):
        copy.wait_recv()

    @pl.loop(*pieces[0])
    def _(j):
        col = pl.ds(pl.multiple_of(j * TILE_D, TILE_D), TILE_D)
        y_ref[:, col] = (own[j] + by_mrg[j].astype(F32)).astype(BF16)

    for copy in merged(0):
        copy.wait_send()
    for copy in merged(1):
        copy.wait_recv()
    for copy in merged(1):
        copy.wait_send()


def finish(y_ref, own, by_mrg, out_ref, piece, sem):
    done = own.shape[0] - BACK
    col = pl.ds(0, done * TILE_D)
    copies = [pltpu.make_async_copy(y_ref.at[:, col], out_ref.at[:, col], sem.at[BACK])]
    copies[0].start()
    for k in range(BACK):
        j = done + k
        piece[k] = (own[j] + by_mrg[j].astype(F32)).astype(BF16)
        copies.append(pltpu.make_async_copy(piece.at[k], out_ref.at[:, pl.ds(j * TILE_D, TILE_D)], sem.at[k]))
        copies[-1].start()
    for copy in copies:
        copy.wait()


def solution(mesh):
    n = mesh.shape["tp"]

    def step(x, w_gate, w_up, w_down):
        rows, d = x.shape
        ff = w_gate.shape[1]
        n_d = d // TILE_D
        dma = pltpu.SemaphoreType.DMA
        pieces = (n_d, rows, TILE_D)
        vmem = pl.BlockSpec(memory_space=pltpu.VMEM)
        parts = pl.pallas_call(
            functools.partial(kernel, n),
            out_shape=(pltpu.VMEM((rows, d), BF16), pltpu.VMEM(pieces, F32), pltpu.VMEM(pieces, BF16)),
            in_specs=[pl.BlockSpec(memory_space=pl.ANY)] * 4,
            out_specs=(vmem, vmem, vmem),
            scratch_shapes=[
                pltpu.VMEM((n, rows, d), BF16),
                pltpu.VMEM((2, rows, ff), BF16),
                pltpu.VMEM((SLOTS_H, d, TILE_H), BF16),
                pltpu.VMEM((SLOTS_H, d, TILE_H), BF16),
                pltpu.VMEM((SLOTS_D, ff, TILE_D), BF16),
                pltpu.VMEM(pieces, F32),
                pltpu.VMEM(pieces, BF16),
                pltpu.VMEM(pieces, BF16),
                pltpu.VMEM(pieces, BF16),
                pltpu.VMEM(pieces, BF16),
                pltpu.VMEM(pieces, BF16),
                dma((2,)), dma((SLOTS_H,)), dma((SLOTS_H,)), dma((SLOTS_D,)),
                dma((6,)), dma((6,)), dma((2,)), dma((2,)),
                dma((2, 2)), dma((2, 2)), dma((2, 2)), dma((2, 2)),
            ],
            compiler_params=pltpu.CompilerParams(
                collective_id=0, has_side_effects=True, vmem_limit_bytes=VMEM_MIB * 1024 * 1024
            ),
            cost_estimate=pl.CostEstimate(
                flops=6 * n * rows * d * ff, bytes_accessed=6 * n * d * ff, transcendentals=n * rows * ff
            ),
            name="mlp_ring",
        )(x, w_gate, w_up, w_down)
        return pl.pallas_call(
            finish,
            out_shape=jax.ShapeDtypeStruct((rows, d), BF16),
            in_specs=[vmem] * 3,
            out_specs=pl.BlockSpec(memory_space=pl.ANY),
            scratch_shapes=[pltpu.VMEM((BACK, rows, TILE_D), BF16), dma((BACK + 1,))],
            compiler_params=pltpu.CompilerParams(vmem_limit_bytes=FINISH_MIB * 1024 * 1024),
            name="finish",
        )(*parts)

    return jax.shard_map(
        step,
        mesh=mesh,
        in_specs=(P(("dp", "tp"), None), P(None, "tp"), P(None, "tp"), P("tp", None)),
        out_specs=P(("dp", "tp"), None),
        check_vma=False,
    )
```

```python
import functools

import jax
import jax.numpy as jnp
from jax import lax
from jax.experimental import pallas as pl
from jax.experimental.pallas import tpu as pltpu
from jax.sharding import PartitionSpec as P

MESH = pl.DeviceIdType.MESH
F32 = jnp.float32
BF16 = jnp.bfloat16

TILE_H = 256
TILE_D = 512
BACK = 2
SLOTS_H = 3
SLOTS_D = 3
VMEM_MIB = 48
FINISH_MIB = 4

OWN, FIRST, SECOND, FAR = range(4)


def kernel(
    n,
    x_ref, wg_ref, wu_ref, wd_ref, y_ref, own, by_mrg,
    xs, hid, wg, wu, wd, mid, to_dir, to_far, to_mrg, by_dir, by_far,
    x_sem, wg_sem, wu_sem, wd_sem, ag_send, ag_recv, dir_send, dir_recv, far_send, far_recv, mrg_send, mrg_recv,
):
    me = lax.axis_index("tp")
    right, left = lax.rem(me + 1, n), lax.rem(me + n - 1, n)
    rows, d = x_ref.shape
    half = rows // 2
    n_h = wg_ref.shape[1] // TILE_H
    n_d = d // TILE_D
    pieces = ((0, n_d - BACK), (n_d - BACK, n_d))
    passes = xs.shape[0]
    a, b = pl.ds(0, half), pl.ds(half, half)

    def load_h(g):
        col = pl.ds(pl.multiple_of(lax.rem(g, n_h) * TILE_H, TILE_H), TILE_H)
        s = lax.rem(g, SLOTS_H)
        return (
            pltpu.make_async_copy(wg_ref.at[:, col], wg.at[s], wg_sem.at[s]),
            pltpu.make_async_copy(wu_ref.at[:, col], wu.at[s], wu_sem.at[s]),
        )

    def load_d(g):
        col = pl.ds(pl.multiple_of(lax.rem(g, n_d) * TILE_D, TILE_D), TILE_D)
        s = lax.rem(g, SLOTS_D)
        return pltpu.make_async_copy(wd_ref.at[:, col], wd.at[s], wd_sem.at[s])

    def send(src, dst, send_sem, recv_sem, to):
        return pltpu.make_async_remote_copy(
            src_ref=src, dst_ref=dst, send_sem=send_sem, recv_sem=recv_sem, device_id={"tp": to}, device_id_type=MESH
        )

    barrier = pltpu.get_barrier_semaphore()
    for neighbour in (left, right):
        pl.semaphore_signal(barrier, inc=1, device_id={"tp": neighbour}, device_id_type=MESH)
    pl.semaphore_wait(barrier, 2)

    heads = [
        send(x_ref.at[a], xs.at[FIRST, a], ag_send.at[0], ag_recv.at[0], right),
        send(x_ref.at[b], xs.at[FIRST, b], ag_send.at[1], ag_recv.at[1], left),
    ]
    tails = [
        send(xs.at[OWN, b], xs.at[SECOND, a], ag_send.at[2], ag_recv.at[2], right),
        send(xs.at[OWN, a], xs.at[SECOND, b], ag_send.at[3], ag_recv.at[3], left),
    ]
    onward = [
        send(xs.at[FIRST, a], xs.at[FAR, a], ag_send.at[4], ag_recv.at[4], right),
        send(xs.at[FIRST, b], xs.at[FAR, b], ag_send.at[5], ag_recv.at[5], left),
    ]
    direct = [
        send(to_dir.at[:, b], by_dir.at[:, b], dir_send.at[0], dir_recv.at[0], right),
        send(to_dir.at[:, a], by_dir.at[:, a], dir_send.at[1], dir_recv.at[1], left),
    ]

    def far(p):
        t = pl.ds(pieces[p][0], pieces[p][1] - pieces[p][0])
        return (
            send(to_far.at[t, a], by_far.at[t, b], far_send.at[p, 0], far_recv.at[p, 0], right),
            send(to_far.at[t, b], by_far.at[t, a], far_send.at[p, 1], far_recv.at[p, 1], left),
        )

    def merged(p):
        t = pl.ds(pieces[p][0], pieces[p][1] - pieces[p][0])
        return (
            send(to_mrg.at[t, b], by_mrg.at[t, a], mrg_send.at[p, 0], mrg_recv.at[p, 0], right),
            send(to_mrg.at[t, a], by_mrg.at[t, b], mrg_send.at[p, 1], mrg_recv.at[p, 1], left),
        )

    for copy in heads:
        copy.start()
    own_x = pltpu.make_async_copy(x_ref, xs.at[OWN], x_sem)
    own_x.start()
    own_x.wait()
    for copy in tails:
        copy.start()

    for g in range(SLOTS_H):
        for copy in load_h(g):
            copy.start()
    for g in range(SLOTS_D):
        load_d(g).start()

    def hidden(p):
        @pl.loop(0, n_h)
        def _(i):
            g = p * n_h + i
            s = lax.rem(g, SLOTS_H)
            for copy in load_h(g):
                copy.wait()
            gate = jnp.dot(xs[p], wg[s], preferred_element_type=F32)
            up = jnp.dot(xs[p], wu[s], preferred_element_type=F32)
            col = pl.ds(pl.multiple_of(i * TILE_H, TILE_H), TILE_H)
            hid[min(p, 1), :, col] = (jax.nn.gelu(gate) * up).astype(BF16)

            @pl.when(g + SLOTS_H < passes * n_h)
            def _():
                for copy in load_h(g + SLOTS_H):
                    copy.start()

    def down(turn, p, put):
        @pl.loop(0, n_d)
        def _(j):
            g = turn * n_d + j
            s = lax.rem(g, SLOTS_D)
            load_d(g).wait()
            put(j, jnp.dot(hid[min(p, 1)], wd[s], preferred_element_type=F32))

            @pl.when(g + SLOTS_D < passes * n_d)
            def _():
                load_d(g + SLOTS_D).start()

    def put_own(j, term):
        own[j] = term

    def put_direct(j, term):
        to_dir[j] = term.astype(BF16)

    def put_mid(j, term):
        mid[j] = term

    def put_far(j, term):
        to_far[j] = term.astype(BF16)

        for p, (_, end) in enumerate(pieces):

            @pl.when(j == end - 1)
            def _():
                for copy in far(p):
                    copy.start()

    hidden(OWN)

    for copy in heads:
        copy.wait_recv()
    for copy in onward:
        copy.start()
    hidden(FIRST)
    down(0, FIRST, put_direct)
    for copy in direct:
        copy.start()

    for copy in tails:
        copy.wait_recv()
    hidden(SECOND)
    down(1, SECOND, put_mid)

    for copy in onward:
        copy.wait_recv()
    hidden(FAR)
    down(2, FAR, put_far)
    down(3, OWN, put_own)

    for p, (start, end) in enumerate(pieces):
        for copy in far(p):
            copy.wait_recv()

        @pl.loop(start, end)
        def _(j):
            to_mrg[j] = (mid[j] + by_far[j].astype(F32)).astype(BF16)

        for copy in merged(p):
            copy.start()

    for copy in direct:
        copy.wait_recv()

    @pl.loop(0, n_d)
    def _(j):
        own[j] += by_dir[j].astype(F32)

    for copy in heads + tails + onward + [*direct, *far(0), *far(1)]:
        copy.wait_send()
    for copy in merged(0):
        copy.wait_recv()

    @pl.loop(*pieces[0])
    def _(j):
        col = pl.ds(pl.multiple_of(j * TILE_D, TILE_D), TILE_D)
        y_ref[:, col] = (own[j] + by_mrg[j].astype(F32)).astype(BF16)

    for copy in merged(0):
        copy.wait_send()
    for copy in merged(1):
        copy.wait_recv()
    for copy in merged(1):
        copy.wait_send()


def finish(y_ref, own, by_mrg, out_ref, back, sem):
    n_d = own.shape[0]
    done = (n_d - BACK) * TILE_D
    first, second = pl.ds(0, done), pl.ds(done, BACK * TILE_D)
    copies = [
        pltpu.make_async_copy(y_ref.at[:, first], out_ref.at[:, first], sem.at[0]),
        pltpu.make_async_copy(back, out_ref.at[:, second], sem.at[1]),
    ]
    copies[0].start()
    for k in range(BACK):
        j = n_d - BACK + k
        back[:, pl.ds(k * TILE_D, TILE_D)] = (own[j] + by_mrg[j].astype(F32)).astype(BF16)
    copies[1].start()
    for copy in copies:
        copy.wait()


def solution(mesh):
    n = mesh.shape["tp"]

    def step(x, w_gate, w_up, w_down):
        rows, d = x.shape
        ff = w_gate.shape[1]
        n_d = d // TILE_D
        dma = pltpu.SemaphoreType.DMA
        pieces = (n_d, rows, TILE_D)
        vmem = pl.BlockSpec(memory_space=pltpu.VMEM)
        parts = pl.pallas_call(
            functools.partial(kernel, n),
            out_shape=(pltpu.VMEM((rows, d), BF16), pltpu.VMEM(pieces, F32), pltpu.VMEM(pieces, BF16)),
            in_specs=[pl.BlockSpec(memory_space=pl.ANY)] * 4,
            out_specs=(vmem, vmem, vmem),
            scratch_shapes=[
                pltpu.VMEM((n, rows, d), BF16),
                pltpu.VMEM((2, rows, ff), BF16),
                pltpu.VMEM((SLOTS_H, d, TILE_H), BF16),
                pltpu.VMEM((SLOTS_H, d, TILE_H), BF16),
                pltpu.VMEM((SLOTS_D, ff, TILE_D), BF16),
                pltpu.VMEM(pieces, F32),
                pltpu.VMEM(pieces, BF16),
                pltpu.VMEM(pieces, BF16),
                pltpu.VMEM(pieces, BF16),
                pltpu.VMEM(pieces, BF16),
                pltpu.VMEM(pieces, BF16),
                dma, dma((SLOTS_H,)), dma((SLOTS_H,)), dma((SLOTS_D,)),
                dma((6,)), dma((6,)), dma((2,)), dma((2,)),
                dma((2, 2)), dma((2, 2)), dma((2, 2)), dma((2, 2)),
            ],
            compiler_params=pltpu.CompilerParams(
                collective_id=0, has_side_effects=True, vmem_limit_bytes=VMEM_MIB * 1024 * 1024
            ),
            cost_estimate=pl.CostEstimate(
                flops=6 * n * rows * d * ff, bytes_accessed=6 * n * d * ff, transcendentals=n * rows * ff
            ),
            name="mlp_ring",
        )(x, w_gate, w_up, w_down)
        return pl.pallas_call(
            finish,
            out_shape=jax.ShapeDtypeStruct((rows, d), BF16),
            in_specs=[vmem] * 3,
            out_specs=pl.BlockSpec(memory_space=pl.ANY),
            scratch_shapes=[pltpu.VMEM((rows, BACK * TILE_D), BF16), dma((2,))],
            compiler_params=pltpu.CompilerParams(vmem_limit_bytes=FINISH_MIB * 1024 * 1024),
            name="finish",
        )(*parts)

    return jax.shard_map(
        step,
        mesh=mesh,
        in_specs=(P(("dp", "tp"), None), P(None, "tp"), P(None, "tp"), P("tp", None)),
        out_specs=P(("dp", "tp"), None),
        check_vma=False,
    )
```

```python
import functools

import jax
import jax.numpy as jnp
from jax import lax
from jax.experimental import pallas as pl
from jax.experimental.pallas import tpu as pltpu
from jax.sharding import PartitionSpec as P

MESH = pl.DeviceIdType.MESH
F32 = jnp.float32
BF16 = jnp.bfloat16

TILE_H = 256
TILE_D = 512
BACK = 2
SLOTS_H = 3
SLOTS_D = 3
VMEM_MIB = 48
FINISH_MIB = 4

OWN, FIRST, SECOND, FAR = range(4)


def kernel(
    n,
    x_ref, wg_ref, wu_ref, wd_ref, y_ref, own, by_mrg,
    xs, hid, wg, wu, wd, mid, to_dir, to_far, to_mrg, by_dir, by_far,
    x_sem, wg_sem, wu_sem, wd_sem, ag_send, ag_recv, dir_send, dir_recv, far_send, far_recv, mrg_send, mrg_recv,
):
    me = lax.axis_index("tp")
    right, left = lax.rem(me + 1, n), lax.rem(me + n - 1, n)
    rows, d = x_ref.shape
    half = rows // 2
    n_h = wg_ref.shape[1] // TILE_H
    n_d = d // TILE_D
    pieces = ((0, n_d - BACK), (n_d - BACK, n_d))
    passes = xs.shape[0]
    a, b = pl.ds(0, half), pl.ds(half, half)

    def load_h(g):
        col = pl.ds(pl.multiple_of(lax.rem(g, n_h) * TILE_H, TILE_H), TILE_H)
        s = lax.rem(g, SLOTS_H)
        return (
            pltpu.make_async_copy(wg_ref.at[:, col], wg.at[s], wg_sem.at[s]),
            pltpu.make_async_copy(wu_ref.at[:, col], wu.at[s], wu_sem.at[s]),
        )

    def load_d(g):
        col = pl.ds(pl.multiple_of(lax.rem(g, n_d) * TILE_D, TILE_D), TILE_D)
        s = lax.rem(g, SLOTS_D)
        return pltpu.make_async_copy(wd_ref.at[:, col], wd.at[s], wd_sem.at[s])

    def send(src, dst, send_sem, recv_sem, to):
        return pltpu.make_async_remote_copy(
            src_ref=src, dst_ref=dst, send_sem=send_sem, recv_sem=recv_sem, device_id={"tp": to}, device_id_type=MESH
        )

    barrier = pltpu.get_barrier_semaphore()
    for neighbour in (left, right):
        pl.semaphore_signal(barrier, inc=1, device_id={"tp": neighbour}, device_id_type=MESH)
    own_x = pltpu.make_async_copy(x_ref, xs.at[OWN], x_sem)
    own_x.start()
    pl.semaphore_wait(barrier, 2)

    heads = [
        send(x_ref.at[a], xs.at[FIRST, a], ag_send.at[0], ag_recv.at[0], right),
        send(x_ref.at[b], xs.at[FIRST, b], ag_send.at[1], ag_recv.at[1], left),
    ]
    tails = [
        send(xs.at[OWN, b], xs.at[SECOND, a], ag_send.at[2], ag_recv.at[2], right),
        send(xs.at[OWN, a], xs.at[SECOND, b], ag_send.at[3], ag_recv.at[3], left),
    ]
    onward = [
        send(xs.at[FIRST, a], xs.at[FAR, a], ag_send.at[4], ag_recv.at[4], right),
        send(xs.at[FIRST, b], xs.at[FAR, b], ag_send.at[5], ag_recv.at[5], left),
    ]
    direct = [
        send(to_dir.at[1], by_dir.at[1], dir_send.at[0], dir_recv.at[0], right),
        send(to_dir.at[0], by_dir.at[0], dir_send.at[1], dir_recv.at[1], left),
    ]

    def far(p):
        t = pl.ds(pieces[p][0], pieces[p][1] - pieces[p][0])
        return (
            send(to_far.at[0, t], by_far.at[1, t], far_send.at[p, 0], far_recv.at[p, 0], right),
            send(to_far.at[1, t], by_far.at[0, t], far_send.at[p, 1], far_recv.at[p, 1], left),
        )

    def merged(p):
        t = pl.ds(pieces[p][0], pieces[p][1] - pieces[p][0])
        return (
            send(to_mrg.at[1, t], by_mrg.at[0, t], mrg_send.at[p, 0], mrg_recv.at[p, 0], right),
            send(to_mrg.at[0, t], by_mrg.at[1, t], mrg_send.at[p, 1], mrg_recv.at[p, 1], left),
        )

    for copy in heads:
        copy.start()
    own_x.wait()
    for copy in tails:
        copy.start()

    for g in range(SLOTS_H):
        for copy in load_h(g):
            copy.start()
    for g in range(SLOTS_D):
        load_d(g).start()

    def hidden(p):
        @pl.loop(0, n_h)
        def _(i):
            g = p * n_h + i
            s = lax.rem(g, SLOTS_H)
            for copy in load_h(g):
                copy.wait()
            gate = jnp.dot(xs[p], wg[s], preferred_element_type=F32)
            up = jnp.dot(xs[p], wu[s], preferred_element_type=F32)
            col = pl.ds(pl.multiple_of(i * TILE_H, TILE_H), TILE_H)
            hid[min(p, 1), :, col] = (jax.nn.gelu(gate) * up).astype(BF16)

            @pl.when(g + SLOTS_H < passes * n_h)
            def _():
                for copy in load_h(g + SLOTS_H):
                    copy.start()

    def down(turn, p, put):
        @pl.loop(0, n_d)
        def _(j):
            g = turn * n_d + j
            s = lax.rem(g, SLOTS_D)
            load_d(g).wait()
            put(j, jnp.dot(hid[min(p, 1)], wd[s], preferred_element_type=F32))

            @pl.when(g + SLOTS_D < passes * n_d)
            def _():
                load_d(g + SLOTS_D).start()

    def put_own(j, term):
        own[j] = term

    def put_direct(j, term):
        for k, h in enumerate((a, b)):
            to_dir[k, j] = term[h.start : h.start + half].astype(BF16)

    def put_mid(j, term):
        mid[j] = term

    def put_far(j, term):
        for k, h in enumerate((a, b)):
            to_far[k, j] = term[h.start : h.start + half].astype(BF16)

        for p, (_, end) in enumerate(pieces):

            @pl.when(j == end - 1)
            def _():
                for copy in far(p):
                    copy.start()

    hidden(OWN)

    for copy in heads:
        copy.wait_recv()
    for copy in onward:
        copy.start()
    hidden(FIRST)
    down(0, FIRST, put_direct)
    for copy in direct:
        copy.start()

    for copy in tails:
        copy.wait_recv()
    hidden(SECOND)
    down(1, SECOND, put_mid)

    for copy in onward:
        copy.wait_recv()
    hidden(FAR)
    down(2, FAR, put_far)
    down(3, OWN, put_own)

    for p, (start, end) in enumerate(pieces):
        for copy in far(p):
            copy.wait_recv()

        @pl.loop(start, end)
        def _(j):
            for k, h in enumerate((a, b)):
                to_mrg[k, j] = (mid[j, h] + by_far[k, j].astype(F32)).astype(BF16)

        for copy in merged(p):
            copy.start()

    for copy in direct:
        copy.wait_recv()

    @pl.loop(0, n_d)
    def _(j):
        for k, h in enumerate((a, b)):
            own[j, h] += by_dir[k, j].astype(F32)

    for copy in heads + tails + onward + [*direct, *far(0), *far(1)]:
        copy.wait_send()
    for copy in merged(0):
        copy.wait_recv()

    @pl.loop(*pieces[0])
    def _(j):
        col = pl.ds(pl.multiple_of(j * TILE_D, TILE_D), TILE_D)
        for k, h in enumerate((a, b)):
            y_ref[h, col] = (own[j, h] + by_mrg[k, j].astype(F32)).astype(BF16)

    for copy in merged(0):
        copy.wait_send()
    for copy in merged(1):
        copy.wait_recv()
    for copy in merged(1):
        copy.wait_send()


def finish(y_ref, own, by_mrg, out_ref, piece, sem):
    done = own.shape[0] - BACK
    col = pl.ds(0, done * TILE_D)
    copies = [pltpu.make_async_copy(y_ref.at[:, col], out_ref.at[:, col], sem.at[BACK])]
    copies[0].start()
    for k in range(BACK):
        j = done + k
        half = by_mrg.shape[2]
        for i in range(2):
            h = pl.ds(i * half, half)
            piece[k, h] = (own[j, h] + by_mrg[i, j].astype(F32)).astype(BF16)
        copies.append(pltpu.make_async_copy(piece.at[k], out_ref.at[:, pl.ds(j * TILE_D, TILE_D)], sem.at[k]))
        copies[-1].start()
    for copy in copies:
        copy.wait()


def solution(mesh):
    n = mesh.shape["tp"]

    def step(x, w_gate, w_up, w_down):
        rows, d = x.shape
        ff = w_gate.shape[1]
        n_d = d // TILE_D
        dma = pltpu.SemaphoreType.DMA
        terms = (n_d, rows, TILE_D)
        halves = (2, n_d, rows // 2, TILE_D)
        vmem = pl.BlockSpec(memory_space=pltpu.VMEM)
        parts = pl.pallas_call(
            functools.partial(kernel, n),
            out_shape=(pltpu.VMEM((rows, d), BF16), pltpu.VMEM(terms, F32), pltpu.VMEM(halves, BF16)),
            in_specs=[pl.BlockSpec(memory_space=pl.ANY)] * 4,
            out_specs=(vmem, vmem, vmem),
            scratch_shapes=[
                pltpu.VMEM((n, rows, d), BF16),
                pltpu.VMEM((2, rows, ff), BF16),
                pltpu.VMEM((SLOTS_H, d, TILE_H), BF16),
                pltpu.VMEM((SLOTS_H, d, TILE_H), BF16),
                pltpu.VMEM((SLOTS_D, ff, TILE_D), BF16),
                pltpu.VMEM(terms, F32),
                pltpu.VMEM(halves, BF16),
                pltpu.VMEM(halves, BF16),
                pltpu.VMEM(halves, BF16),
                pltpu.VMEM(halves, BF16),
                pltpu.VMEM(halves, BF16),
                dma, dma((SLOTS_H,)), dma((SLOTS_H,)), dma((SLOTS_D,)),
                dma((6,)), dma((6,)), dma((2,)), dma((2,)),
                dma((2, 2)), dma((2, 2)), dma((2, 2)), dma((2, 2)),
            ],
            compiler_params=pltpu.CompilerParams(
                collective_id=0, has_side_effects=True, vmem_limit_bytes=VMEM_MIB * 1024 * 1024
            ),
            cost_estimate=pl.CostEstimate(
                flops=6 * n * rows * d * ff, bytes_accessed=6 * n * d * ff, transcendentals=n * rows * ff
            ),
            name="mlp_ring",
        )(x, w_gate, w_up, w_down)
        return pl.pallas_call(
            finish,
            out_shape=jax.ShapeDtypeStruct((rows, d), BF16),
            in_specs=[vmem] * 3,
            out_specs=pl.BlockSpec(memory_space=pl.ANY),
            scratch_shapes=[pltpu.VMEM((BACK, rows, TILE_D), BF16), dma((BACK + 1,))],
            compiler_params=pltpu.CompilerParams(vmem_limit_bytes=FINISH_MIB * 1024 * 1024),
            name="finish",
        )(*parts)

    return jax.shard_map(
        step,
        mesh=mesh,
        in_specs=(P(("dp", "tp"), None), P(None, "tp"), P(None, "tp"), P("tp", None)),
        out_specs=P(("dp", "tp"), None),
        check_vma=False,
    )
```

```python
import functools

import jax
import jax.numpy as jnp
from jax import lax
from jax.experimental import pallas as pl
from jax.experimental.pallas import tpu as pltpu
from jax.sharding import PartitionSpec as P

MESH = pl.DeviceIdType.MESH
F32 = jnp.float32
BF16 = jnp.bfloat16

TILE_H = 256
TILE_D = 512
BACK = 2
SLOTS_H = 3
SLOTS_D = 3
VMEM_MIB = 48
FINISH_MIB = 4

OWN, FIRST, SECOND, FAR = range(4)


def kernel(
    n,
    x_ref, wg_ref, wu_ref, wd_ref, y_ref, own, by_mrg,
    xs, hid, wg, wu, wd, mid, to_dir, to_far, to_mrg, by_dir, by_far,
    ready, x_sem, wg_sem, wu_sem, wd_sem, ag_send, ag_recv, dir_send, dir_recv, far_send, far_recv, mrg_send, mrg_recv,
):
    me = lax.axis_index("tp")
    right, left = lax.rem(me + 1, n), lax.rem(me + n - 1, n)
    rows, d = x_ref.shape
    half = rows // 2
    n_h = wg_ref.shape[1] // TILE_H
    n_d = d // TILE_D
    pieces = ((0, n_d - BACK), (n_d - BACK, n_d))
    passes = xs.shape[0]
    a, b = pl.ds(0, half), pl.ds(half, half)

    def load_h(g):
        col = pl.ds(pl.multiple_of(lax.rem(g, n_h) * TILE_H, TILE_H), TILE_H)
        s = lax.rem(g, SLOTS_H)
        return (
            pltpu.make_async_copy(wg_ref.at[:, col], wg.at[s], wg_sem.at[s]),
            pltpu.make_async_copy(wu_ref.at[:, col], wu.at[s], wu_sem.at[s]),
        )

    def load_d(g):
        col = pl.ds(pl.multiple_of(lax.rem(g, n_d) * TILE_D, TILE_D), TILE_D)
        s = lax.rem(g, SLOTS_D)
        return pltpu.make_async_copy(wd_ref.at[:, col], wd.at[s], wd_sem.at[s])

    def send(src, dst, send_sem, recv_sem, to):
        return pltpu.make_async_remote_copy(
            src_ref=src, dst_ref=dst, send_sem=send_sem, recv_sem=recv_sem, device_id={"tp": to}, device_id_type=MESH
        )

    barrier = pltpu.get_barrier_semaphore()
    pl.semaphore_signal(barrier, inc=1, device_id={"tp": left}, device_id_type=MESH)
    own_x = pltpu.make_async_copy(x_ref, xs.at[OWN], x_sem)
    own_x.start()
    pl.semaphore_wait(barrier, 1)

    heads = [
        send(x_ref.at[a], xs.at[FIRST, a], ag_send.at[0], ag_recv.at[0], right),
        send(x_ref.at[b], xs.at[FIRST, b], ag_send.at[1], ag_recv.at[1], left),
    ]
    tails = [
        send(xs.at[OWN, b], xs.at[SECOND, a], ag_send.at[2], ag_recv.at[2], right),
        send(xs.at[OWN, a], xs.at[SECOND, b], ag_send.at[3], ag_recv.at[3], left),
    ]
    onward = [
        send(xs.at[FIRST, a], xs.at[FAR, a], ag_send.at[4], ag_recv.at[4], right),
        send(xs.at[FIRST, b], xs.at[FAR, b], ag_send.at[5], ag_recv.at[5], left),
    ]
    direct = [
        send(to_dir.at[1], by_dir.at[1], dir_send.at[0], dir_recv.at[0], right),
        send(to_dir.at[0], by_dir.at[0], dir_send.at[1], dir_recv.at[1], left),
    ]

    def far(p):
        t = pl.ds(pieces[p][0], pieces[p][1] - pieces[p][0])
        return (
            send(to_far.at[0, t], by_far.at[1, t], far_send.at[p, 0], far_recv.at[p, 0], right),
            send(to_far.at[1, t], by_far.at[0, t], far_send.at[p, 1], far_recv.at[p, 1], left),
        )

    def merged(p):
        t = pl.ds(pieces[p][0], pieces[p][1] - pieces[p][0])
        return (
            send(to_mrg.at[1, t], by_mrg.at[0, t], mrg_send.at[p, 0], mrg_recv.at[p, 0], right),
            send(to_mrg.at[0, t], by_mrg.at[1, t], mrg_send.at[p, 1], mrg_recv.at[p, 1], left),
        )

    pl.semaphore_signal(ready, inc=1, device_id={"tp": right}, device_id_type=MESH)
    heads[0].start()
    pl.semaphore_wait(ready, 1)
    heads[1].start()
    own_x.wait()
    for copy in tails:
        copy.start()

    for g in range(SLOTS_H):
        for copy in load_h(g):
            copy.start()
    for g in range(SLOTS_D):
        load_d(g).start()

    def hidden(p):
        @pl.loop(0, n_h)
        def _(i):
            g = p * n_h + i
            s = lax.rem(g, SLOTS_H)
            for copy in load_h(g):
                copy.wait()
            gate = jnp.dot(xs[p], wg[s], preferred_element_type=F32)
            up = jnp.dot(xs[p], wu[s], preferred_element_type=F32)
            col = pl.ds(pl.multiple_of(i * TILE_H, TILE_H), TILE_H)
            hid[min(p, 1), :, col] = (jax.nn.gelu(gate) * up).astype(BF16)

            @pl.when(g + SLOTS_H < passes * n_h)
            def _():
                for copy in load_h(g + SLOTS_H):
                    copy.start()

    def down(turn, p, put):
        @pl.loop(0, n_d)
        def _(j):
            g = turn * n_d + j
            s = lax.rem(g, SLOTS_D)
            load_d(g).wait()
            put(j, jnp.dot(hid[min(p, 1)], wd[s], preferred_element_type=F32))

            @pl.when(g + SLOTS_D < passes * n_d)
            def _():
                load_d(g + SLOTS_D).start()

    def put_own(j, term):
        own[j] = term

    def put_direct(j, term):
        for k, h in enumerate((a, b)):
            to_dir[k, j] = term[h.start : h.start + half].astype(BF16)

    def put_mid(j, term):
        mid[j] = term

    def put_far(j, term):
        for k, h in enumerate((a, b)):
            to_far[k, j] = term[h.start : h.start + half].astype(BF16)

        for p, (_, end) in enumerate(pieces):

            @pl.when(j == end - 1)
            def _():
                for copy in far(p):
                    copy.start()

    hidden(OWN)

    for copy in heads:
        copy.wait_recv()
    for copy in onward:
        copy.start()
    hidden(FIRST)
    down(0, FIRST, put_direct)
    for copy in direct:
        copy.start()

    for copy in tails:
        copy.wait_recv()
    hidden(SECOND)
    down(1, SECOND, put_mid)

    for copy in onward:
        copy.wait_recv()
    hidden(FAR)
    down(2, FAR, put_far)
    down(3, OWN, put_own)

    for p, (start, end) in enumerate(pieces):
        for copy in far(p):
            copy.wait_recv()

        @pl.loop(start, end)
        def _(j):
            for k, h in enumerate((a, b)):
                to_mrg[k, j] = (mid[j, h] + by_far[k, j].astype(F32)).astype(BF16)

        for copy in merged(p):
            copy.start()

    for copy in direct:
        copy.wait_recv()

    @pl.loop(0, n_d)
    def _(j):
        for k, h in enumerate((a, b)):
            own[j, h] += by_dir[k, j].astype(F32)

    for copy in heads + tails + onward + [*direct, *far(0), *far(1)]:
        copy.wait_send()
    for copy in merged(0):
        copy.wait_recv()

    @pl.loop(*pieces[0])
    def _(j):
        col = pl.ds(pl.multiple_of(j * TILE_D, TILE_D), TILE_D)
        for k, h in enumerate((a, b)):
            y_ref[h, col] = (own[j, h] + by_mrg[k, j].astype(F32)).astype(BF16)

    for copy in merged(0):
        copy.wait_send()
    for copy in merged(1):
        copy.wait_recv()
    for copy in merged(1):
        copy.wait_send()


def finish(y_ref, own, by_mrg, out_ref, piece, sem):
    done = own.shape[0] - BACK
    col = pl.ds(0, done * TILE_D)
    copies = [pltpu.make_async_copy(y_ref.at[:, col], out_ref.at[:, col], sem.at[BACK])]
    copies[0].start()
    for k in range(BACK):
        j = done + k
        half = by_mrg.shape[2]
        for i in range(2):
            h = pl.ds(i * half, half)
            piece[k, h] = (own[j, h] + by_mrg[i, j].astype(F32)).astype(BF16)
        copies.append(pltpu.make_async_copy(piece.at[k], out_ref.at[:, pl.ds(j * TILE_D, TILE_D)], sem.at[k]))
        copies[-1].start()
    for copy in copies:
        copy.wait()


def solution(mesh):
    n = mesh.shape["tp"]

    def step(x, w_gate, w_up, w_down):
        rows, d = x.shape
        ff = w_gate.shape[1]
        n_d = d // TILE_D
        dma = pltpu.SemaphoreType.DMA
        terms = (n_d, rows, TILE_D)
        halves = (2, n_d, rows // 2, TILE_D)
        vmem = pl.BlockSpec(memory_space=pltpu.VMEM)
        parts = pl.pallas_call(
            functools.partial(kernel, n),
            out_shape=(pltpu.VMEM((rows, d), BF16), pltpu.VMEM(terms, F32), pltpu.VMEM(halves, BF16)),
            in_specs=[pl.BlockSpec(memory_space=pl.ANY)] * 4,
            out_specs=(vmem, vmem, vmem),
            scratch_shapes=[
                pltpu.VMEM((n, rows, d), BF16),
                pltpu.VMEM((2, rows, ff), BF16),
                pltpu.VMEM((SLOTS_H, d, TILE_H), BF16),
                pltpu.VMEM((SLOTS_H, d, TILE_H), BF16),
                pltpu.VMEM((SLOTS_D, ff, TILE_D), BF16),
                pltpu.VMEM(terms, F32),
                pltpu.VMEM(halves, BF16),
                pltpu.VMEM(halves, BF16),
                pltpu.VMEM(halves, BF16),
                pltpu.VMEM(halves, BF16),
                pltpu.VMEM(halves, BF16),
                pltpu.SemaphoreType.REGULAR, dma, dma((SLOTS_H,)), dma((SLOTS_H,)), dma((SLOTS_D,)),
                dma((6,)), dma((6,)), dma((2,)), dma((2,)),
                dma((2, 2)), dma((2, 2)), dma((2, 2)), dma((2, 2)),
            ],
            compiler_params=pltpu.CompilerParams(
                collective_id=0, has_side_effects=True, vmem_limit_bytes=VMEM_MIB * 1024 * 1024
            ),
            cost_estimate=pl.CostEstimate(
                flops=6 * n * rows * d * ff, bytes_accessed=6 * n * d * ff, transcendentals=n * rows * ff
            ),
            name="mlp_ring",
        )(x, w_gate, w_up, w_down)
        return pl.pallas_call(
            finish,
            out_shape=jax.ShapeDtypeStruct((rows, d), BF16),
            in_specs=[vmem] * 3,
            out_specs=pl.BlockSpec(memory_space=pl.ANY),
            scratch_shapes=[pltpu.VMEM((BACK, rows, TILE_D), BF16), dma((BACK + 1,))],
            compiler_params=pltpu.CompilerParams(vmem_limit_bytes=FINISH_MIB * 1024 * 1024),
            name="finish",
        )(*parts)

    return jax.shard_map(
        step,
        mesh=mesh,
        in_specs=(P(("dp", "tp"), None), P(None, "tp"), P(None, "tp"), P("tp", None)),
        out_specs=P(("dp", "tp"), None),
        check_vma=False,
    )
```

```python
import functools

import jax
import jax.numpy as jnp
from jax import lax
from jax.experimental import pallas as pl
from jax.experimental.pallas import tpu as pltpu
from jax.sharding import PartitionSpec as P

MESH = pl.DeviceIdType.MESH
F32 = jnp.float32
BF16 = jnp.bfloat16

TILE_H = 256
TILE_D = 512
BACK = 2
SLOTS_H = 3
SLOTS_D = 3
VMEM_MIB = 48
FINISH_MIB = 4

OWN, FIRST, SECOND, FAR = range(4)


def kernel(
    n,
    x_ref, wg_ref, wu_ref, wd_ref, y_ref, own, by_mrg,
    xs, hid, wgu, wd, mid, to_dir, to_far, to_mrg, by_dir, by_far,
    ready, h_sem, d_sem, sent, ag_got, dir_got, far_got, mrg_got,
):
    me = lax.axis_index("tp")
    right, left = lax.rem(me + 1, n), lax.rem(me + n - 1, n)
    rows, d = x_ref.shape
    half = rows // 2
    n_h = wg_ref.shape[1] // TILE_H
    n_d = d // TILE_D
    pieces = ((0, n_d - BACK), (n_d - BACK, n_d))
    passes = xs.shape[0]
    a, b = pl.ds(0, half), pl.ds(half, half)

    def load_h(g):
        col = pl.ds(pl.multiple_of(lax.rem(g, n_h) * TILE_H, TILE_H), TILE_H)
        s = lax.rem(g, SLOTS_H)
        for k, w_ref in enumerate((wg_ref, wu_ref)):
            pltpu.make_async_copy(w_ref.at[:, col], wgu.at[s, k], h_sem.at[s]).start()

    def load_d(g):
        col = pl.ds(pl.multiple_of(lax.rem(g, n_d) * TILE_D, TILE_D), TILE_D)
        s = lax.rem(g, SLOTS_D)
        return pltpu.make_async_copy(wd_ref.at[:, col], wd.at[s], d_sem.at[s])

    def wait_all(ref, sem):
        pltpu.make_async_copy(ref, ref, sem).wait()

    def send(src, dst, recv_sem, way):
        return pltpu.make_async_remote_copy(
            src_ref=src,
            dst_ref=dst,
            send_sem=sent.at[way],
            recv_sem=recv_sem,
            device_id={"tp": (right, left)[way]},
            device_id_type=MESH,
        )

    barrier = pltpu.get_barrier_semaphore()
    pl.semaphore_signal(barrier, inc=1, device_id={"tp": left}, device_id_type=MESH)
    own_x = pltpu.make_async_copy(x_ref, xs.at[OWN], d_sem.at[0])
    own_x.start()
    pl.semaphore_wait(barrier, 1)

    heads = [
        send(x_ref.at[a], xs.at[FIRST, a], ag_got.at[0], 0),
        send(x_ref.at[b], xs.at[FIRST, b], ag_got.at[0], 1),
    ]
    tails = [
        send(xs.at[OWN, b], xs.at[SECOND, a], ag_got.at[1], 0),
        send(xs.at[OWN, a], xs.at[SECOND, b], ag_got.at[1], 1),
    ]
    onward = [
        send(xs.at[FIRST, a], xs.at[FAR, a], ag_got.at[2], 0),
        send(xs.at[FIRST, b], xs.at[FAR, b], ag_got.at[2], 1),
    ]
    direct = [
        send(to_dir.at[1], by_dir.at[1], dir_got, 0),
        send(to_dir.at[0], by_dir.at[0], dir_got, 1),
    ]

    def tiles(p):
        return pl.ds(pieces[p][0], pieces[p][1] - pieces[p][0])

    def far(p):
        t = tiles(p)
        return (
            send(to_far.at[0, t], by_far.at[1, t], far_got.at[p], 0),
            send(to_far.at[1, t], by_far.at[0, t], far_got.at[p], 1),
        )

    def merged(p):
        t = tiles(p)
        return (
            send(to_mrg.at[1, t], by_mrg.at[0, t], mrg_got.at[p], 0),
            send(to_mrg.at[0, t], by_mrg.at[1, t], mrg_got.at[p], 1),
        )

    pl.semaphore_signal(ready, inc=1, device_id={"tp": right}, device_id_type=MESH)
    heads[0].start()
    pl.semaphore_wait(ready, 1)
    heads[1].start()
    own_x.wait()
    for copy in tails:
        copy.start()

    for g in range(SLOTS_H):
        load_h(g)
    for g in range(SLOTS_D):
        load_d(g).start()

    def hidden(p):
        @pl.loop(0, n_h)
        def _(i):
            g = p * n_h + i
            s = lax.rem(g, SLOTS_H)
            wait_all(wgu.at[s], h_sem.at[s])
            gate = jnp.dot(xs[p], wgu[s, 0], preferred_element_type=F32)
            up = jnp.dot(xs[p], wgu[s, 1], preferred_element_type=F32)
            col = pl.ds(pl.multiple_of(i * TILE_H, TILE_H), TILE_H)
            hid[min(p, 1), :, col] = (jax.nn.gelu(gate) * up).astype(BF16)

            @pl.when(g + SLOTS_H < passes * n_h)
            def _():
                load_h(g + SLOTS_H)

    def down(turn, p, put):
        @pl.loop(0, n_d)
        def _(j):
            g = turn * n_d + j
            s = lax.rem(g, SLOTS_D)
            load_d(g).wait()
            put(j, jnp.dot(hid[min(p, 1)], wd[s], preferred_element_type=F32))

            @pl.when(g + SLOTS_D < passes * n_d)
            def _():
                load_d(g + SLOTS_D).start()

    def put_own(j, term):
        own[j] = term

    def put_direct(j, term):
        for k, h in enumerate((a, b)):
            to_dir[k, j] = term[h.start : h.start + half].astype(BF16)

    def put_mid(j, term):
        mid[j] = term

    def put_far(j, term):
        for k, h in enumerate((a, b)):
            to_far[k, j] = term[h.start : h.start + half].astype(BF16)

        for p, (_, end) in enumerate(pieces):

            @pl.when(j == end - 1)
            def _():
                for copy in far(p):
                    copy.start()

    hidden(OWN)

    wait_all(xs.at[FIRST], ag_got.at[0])
    for copy in onward:
        copy.start()
    hidden(FIRST)
    down(0, FIRST, put_direct)
    for copy in direct:
        copy.start()

    wait_all(xs.at[SECOND], ag_got.at[1])
    hidden(SECOND)
    down(1, SECOND, put_mid)

    wait_all(xs.at[FAR], ag_got.at[2])
    hidden(FAR)
    down(2, FAR, put_far)
    down(3, OWN, put_own)

    for p, (start, end) in enumerate(pieces):
        wait_all(by_far.at[:, tiles(p)], far_got.at[p])

        @pl.loop(start, end)
        def _(j):
            for k, h in enumerate((a, b)):
                to_mrg[k, j] = (mid[j, h] + by_far[k, j].astype(F32)).astype(BF16)

        for copy in merged(p):
            copy.start()

    wait_all(by_dir, dir_got)

    @pl.loop(0, n_d)
    def _(j):
        for k, h in enumerate((a, b)):
            own[j, h] += by_dir[k, j].astype(F32)

    wait_all(by_mrg.at[:, tiles(0)], mrg_got.at[0])

    @pl.loop(*pieces[0])
    def _(j):
        col = pl.ds(pl.multiple_of(j * TILE_D, TILE_D), TILE_D)
        for k, h in enumerate((a, b)):
            y_ref[h, col] = (own[j, h] + by_mrg[k, j].astype(F32)).astype(BF16)

    wait_all(by_mrg.at[:, tiles(1)], mrg_got.at[1])
    for way in range(2):
        wait_all(xs.at[pl.ds(0, 3)], sent.at[way])


def finish(y_ref, own, by_mrg, out_ref, back, sem):
    n_d, rows, _ = own.shape
    half = rows // 2
    done = (n_d - BACK) * TILE_D
    first, second = pl.ds(0, done), pl.ds(done, BACK * TILE_D)
    pltpu.make_async_copy(y_ref.at[:, first], out_ref.at[:, first], sem).start()
    for k in range(BACK):
        j = n_d - BACK + k
        for i in range(2):
            h = pl.ds(i * half, half)
            back[h, pl.ds(k * TILE_D, TILE_D)] = (own[j, h] + by_mrg[i, j].astype(F32)).astype(BF16)
    pltpu.make_async_copy(back, out_ref.at[:, second], sem).start()
    pltpu.make_async_copy(y_ref, out_ref, sem).wait()


def solution(mesh):
    n = mesh.shape["tp"]

    def step(x, w_gate, w_up, w_down):
        rows, d = x.shape
        ff = w_gate.shape[1]
        n_d = d // TILE_D
        dma = pltpu.SemaphoreType.DMA
        terms = (n_d, rows, TILE_D)
        halves = (2, n_d, rows // 2, TILE_D)
        vmem = pl.BlockSpec(memory_space=pltpu.VMEM)
        parts = pl.pallas_call(
            functools.partial(kernel, n),
            out_shape=(pltpu.VMEM((rows, d), BF16), pltpu.VMEM(terms, F32), pltpu.VMEM(halves, BF16)),
            in_specs=[pl.BlockSpec(memory_space=pl.ANY)] * 4,
            out_specs=(vmem, vmem, vmem),
            scratch_shapes=[
                pltpu.VMEM((n, rows, d), BF16),
                pltpu.VMEM((2, rows, ff), BF16),
                pltpu.VMEM((SLOTS_H, 2, d, TILE_H), BF16),
                pltpu.VMEM((SLOTS_D, ff, TILE_D), BF16),
                pltpu.VMEM(terms, F32),
                pltpu.VMEM(halves, BF16),
                pltpu.VMEM(halves, BF16),
                pltpu.VMEM(halves, BF16),
                pltpu.VMEM(halves, BF16),
                pltpu.VMEM(halves, BF16),
                pltpu.SemaphoreType.REGULAR, dma((SLOTS_H,)), dma((SLOTS_D,)),
                dma((2,)), dma((3,)), dma, dma((2,)), dma((2,)),
            ],
            compiler_params=pltpu.CompilerParams(
                collective_id=0, has_side_effects=True, vmem_limit_bytes=VMEM_MIB * 1024 * 1024
            ),
            cost_estimate=pl.CostEstimate(
                flops=6 * n * rows * d * ff, bytes_accessed=6 * n * d * ff, transcendentals=n * rows * ff
            ),
            name="mlp_ring",
        )(x, w_gate, w_up, w_down)
        return pl.pallas_call(
            finish,
            out_shape=jax.ShapeDtypeStruct((rows, d), BF16),
            in_specs=[vmem] * 3,
            out_specs=pl.BlockSpec(memory_space=pl.ANY),
            scratch_shapes=[pltpu.VMEM((rows, BACK * TILE_D), BF16), dma],
            compiler_params=pltpu.CompilerParams(vmem_limit_bytes=FINISH_MIB * 1024 * 1024),
            name="finish",
        )(*parts)

    return jax.shard_map(
        step,
        mesh=mesh,
        in_specs=(P(("dp", "tp"), None), P(None, "tp"), P(None, "tp"), P("tp", None)),
        out_specs=P(("dp", "tp"), None),
        check_vma=False,
    )
```
